256 devices in a mesh: ta: 128 (over y_lo, x, z, core), aa: 2 (over y_hi).
Axes of the slice: x: 4, y: 4 (y_hi: 2, y_lo: 2; y = y_hi * 2 + y_lo), z: 8, core: 2. Of those that a mesh axis runs over, the one named last changes fastest.
Arguments:
- voltages: bfloat16 [256, 3145728], P('aa', 'ta'), may hold values from -6 to 6
- pfb_window: float32 [4, 8192], replicated, may hold values from -3 to 3
Outputs:
- visibilities: float32 [2048, 256, 512], P('ta', 'aa')
The draws below stay inside these ranges and needn't reach their ends.
All inputs are finite; a program needn't handle non-finite values.
Results may differ from the reference program's by a relative error of at most 0.0026.
Values may be sent and summed in bfloat16 or wider, within the bound.
No kernel may reach another device: no remote copies, remote signals or barrier semaphores. Data moves between devices by JAX's collectives and lax.ppermute only.
A program may use at most 128 MiB of HBM per device.

```python
import math
import jax
import jax.numpy as jnp
from jax import lax

S = 256
NFFT = 8192
CH = 2048
TAPS = 4
FRAMES = 384
CH_OFF = 1024


def steps_of(rng, dims, pieces, least, high):
    gain = 1.0
    for axis_at, blocks in pieces:
        heights = jax.random.uniform(jax.random.fold_in(jax.random.fold_in(rng, 6), axis_at), (blocks,), jnp.float32, least / len(pieces), high / len(pieces))
        gain = gain * jnp.repeat(jnp.exp(heights), dims[axis_at] // blocks).reshape((-1,) + (1,) * (len(dims) - 1 - axis_at))
    return gain


def scatter_about(key, dims, scale, bound, cuts=(), held_as=jnp.bfloat16):
    values = scale * jax.random.normal(key, dims, jnp.float32)
    if cuts:
        values = values * steps_of(key, dims, cuts, -0.22, 0.18)
    return jnp.clip(values, -bound, bound).astype(held_as)


def setup_inputs(seed: int = 0) -> dict:
    streams_of = jax.random.split(jax.random.key(seed), 3)
    return {
        "voltages": scatter_about(streams_of[0], (S, FRAMES * NFFT), 1.0, 6.0, ((0, 2), (1, 128))),
        "pfb_window": scatter_about(streams_of[1], (TAPS, NFFT), 0.5, 3.0, (), jnp.float32),
    }


def reference(voltages, pfb_window):
    frames = voltages.shape[1] // NFFT
    padded = jnp.concatenate([jnp.zeros((S, (TAPS - 1) * NFFT), voltages.dtype), voltages], axis=1)
    window = pfb_window.astype(jnp.float32)

    def one_frame(frame_index):
        start_index = (frame_index * NFFT).astype(jnp.int32)
        samples = lax.dynamic_slice_in_dim(padded, start_index, TAPS * NFFT, 1)
        samples = samples.astype(jnp.float32).reshape(S, TAPS, NFFT)
        filtered = lax.optimization_barrier(jnp.sum(samples * window[None], axis=1))
        spectrum = jnp.fft.rfft(filtered, axis=1)[:, CH_OFF:CH_OFF + CH] / math.sqrt(NFFT)
        stacked = jnp.stack([jnp.real(spectrum), jnp.imag(spectrum)], axis=0).astype(jnp.float32)
        return jnp.transpose(stacked, (2, 0, 1)).astype(jnp.bfloat16)
    spectra = lax.map(one_frame, jnp.arange(frames, dtype=jnp.int32))
    spectra = jnp.transpose(spectra, (1, 0, 2, 3))
    scaling = 1.0 / math.sqrt(frames)
    blocks = spectra.reshape(CH // 16, 16, frames, 2, S)

    def one_block(channel_block):
        values = channel_block.astype(jnp.float32)
        swapped = jnp.stack([values[:, :, 1], -values[:, :, 0]], axis=2)
        left_rows = jnp.concatenate([values, swapped], axis=3)
        result = jnp.einsum('cfpi,cfpj->cij', left_rows, values) * scaling
        return jnp.concatenate([result[:, :S], result[:, S:]], axis=2)
    visible = lax.map(one_block, blocks)
    return visible.reshape(CH, S, 2 * S)
```

```python
import math

import jax
import jax.numpy as jnp
import numpy as np
from jax import lax
from jax.experimental import pallas as pl
from jax.experimental.pallas import tpu as pltpu
from jax.sharding import PartitionSpec as P

NFFT = 8192
CH = 2048
TAPS = 4
CH_OFF = 1024
N1 = 64
N2 = 128
NK = 33
NJ = CH // N1
K2 = CH_OFF // N1
HALF = math.sqrt(0.5)
BF = jnp.bfloat16
F32 = jnp.float32


def twiddle_table():
    phase = np.outer(np.arange(NK), np.arange(N2)) * (2.0 * np.pi / NFFT)
    return np.stack([np.cos(phase), np.sin(phase)], axis=1).astype(np.float32)


def bin_table():
    scale = 1.0 / math.sqrt(NFFT)
    bins = np.arange(K2, K2 + NJ)
    rows = []
    for bin_set, sign in ((bins, 1.0), (-(bins + 1), -1.0)):
        phase = np.outer(bin_set, np.arange(N2)) % N2 * (2.0 * np.pi / N2)
        cosine, sine = np.cos(phase) * scale, np.sin(phase) * scale
        rows.append(np.concatenate([cosine, sine], axis=1))
        rows.append(sign * np.concatenate([-sine, cosine], axis=1))
    table = np.concatenate(rows, axis=0)
    high = table.astype(BF)
    low = (table - high.astype(np.float64)).astype(BF)
    return np.concatenate([high, low], axis=0)


def real_dft8(x):
    s0, d0 = x[0] + x[4], x[0] - x[4]
    s1, d1 = x[1] + x[5], x[1] - x[5]
    s2, d2 = x[2] + x[6], x[2] - x[6]
    s3, d3 = x[3] + x[7], x[3] - x[7]
    e0, e1 = s0 + s2, s1 + s3
    u, v = HALF * (d1 - d3), HALF * (d1 + d3)
    return [(e0 + e1, None), (d0 + u, -(d2 + v)), (s0 - s2, s3 - s1), (d0 - u, d2 - v), (e0 - e1, None)]


def complex_dft8(z, first_half=False):
    sr = [z[j][0] + z[j + 4][0] for j in range(4)]
    si = [z[j][1] + z[j + 4][1] for j in range(4)]
    dr = [z[j][0] - z[j + 4][0] for j in range(4)]
    di = [z[j][1] - z[j + 4][1] for j in range(4)]
    out = [None] * 8
    pr, pi = dr[1], di[1]
    dr[1], di[1] = HALF * (pr + pi), HALF * (pi - pr)
    dr[2], di[2] = di[2], -dr[2]
    pr, pi = dr[3], di[3]
    dr[3], di[3] = HALF * (pi - pr), -HALF * (pr + pi)
    for base, (ar, ai) in ((0, (sr, si)), (1, (dr, di))):
        er, ei = ar[0] + ar[2], ai[0] + ai[2]
        fr, fi = ar[1] + ar[3], ai[1] + ai[3]
        gr, gi = ar[0] - ar[2], ai[0] - ai[2]
        hr, hi = ar[1] - ar[3], ai[1] - ai[3]
        out[base] = (er + fr, ei + fi)
        out[base + 2] = (gr + hi, gi - hr)
        if not first_half:
            out[base + 4] = (er - fr, ei - fi)
            out[base + 6] = (gr - hi, gi + hr)
    return out


def first_half_bins(sections, tw_ref, zhi_ref, zlo_ref, frame, rows):
    def keep(k1, re, im, conj):
        c, s = tw_ref[k1, 0:1, :], tw_ref[k1, 1:2, :]
        if im is None:
            zr, zi = re * c, -(re * s)
        elif conj:
            zr, zi = re * c - im * s, -(im * c + re * s)
        else:
            zr, zi = re * c + im * s, im * c - re * s
        for part, z in ((0, zr), (1, zi)):
            high = z.astype(BF)
            low = (z - high.astype(F32)).astype(BF)
            zhi_ref[k1, rows, part * N2 : (part + 1) * N2] = high
            zlo_ref[k1, rows, part * N2 : (part + 1) * N2] = low

    spectrum = real_dft8([sections[frame, 0, b] for b in range(8)])
    for r in range(5):
        keep(8 * r, spectrum[r][0], spectrum[r][1], False)
    for q in (1, 2, 3):
        z = []
        for b in range(8):
            re, im = sections[frame, 2 * q - 1, b], sections[frame, 2 * q, b]
            if b:
                c, s = math.cos(2 * math.pi * b * q / N1), math.sin(2 * math.pi * b * q / N1)
                re, im = re * c + im * s, im * c - re * s
            z.append((re, im))
        for r, (re, im) in enumerate(complex_dft8(z)):
            k1 = q + 8 * r
            if k1 <= 32:
                keep(k1, re, im, False)
            else:
                keep(N1 - k1, re, im, True)
    z = []
    for b in range(8):
        x = sections[frame, 7, b]
        c, s = math.cos(2 * math.pi * b * 4 / N1), math.sin(2 * math.pi * b * 4 / N1)
        z.append((x * c, x * -s) if b else (x, jnp.zeros_like(x)))
    out = complex_dft8(z, first_half=True)
    for r in range(4):
        keep(4 + 8 * r, out[r][0], out[r][1], False)


def sections_of(frames_of, n_out, w_ref, sections):
    for b in range(8):
        filtered = [[] for _ in range(n_out)]
        for a in range(8):
            n1 = 8 * a + b
            w = [w_ref[k : k + 1, n1 * N2 : (n1 + 1) * N2] for k in range(TAPS)]
            for f, value in enumerate(frames_of(n1, w)):
                filtered[f].append(value)
        for f in range(n_out):
            spectrum = real_dft8(filtered[f])
            sections[f, 0, b] = spectrum[0][0]
            for q in (1, 2, 3):
                sections[f, 2 * q - 1, b] = spectrum[q][0]
                sections[f, 2 * q, b] = spectrum[q][1]
            sections[f, 7, b] = spectrum[4][0]


def frame_at(ref, frame, n1):
    at = frame * NFFT + n1 * N2
    return ref[:, at : at + N2].astype(F32)


def emit_slabs(n_out, table_ref, zhi_ref, zlo_ref, wide_ref, out_ref):
    slab = n_out * 16

    def one(k1, mirror):
        dims = (((1,), (1,)), ((), ()))
        both = lax.dot_general(table_ref[...], zhi_ref[k1], dims, preferred_element_type=F32)
        more = lax.dot_general(table_ref[0:N2, :], zlo_ref[k1], dims, preferred_element_type=F32)
        spectrum = both[:N2] + both[N2:] + more
        for side in range(2 if mirror else 1):
            ch = N1 - k1 if side else k1
            start = (ch // 8) * slab + ch % 8
            for part in range(2):
                at = (side * 2 + part) * NJ
                for f in range(n_out):
                    wide_ref[pl.ds(start + (f * 2 + part) * 8, NJ, stride=8 * slab), :] = spectrum[
                        at : at + NJ, f * N2 : (f + 1) * N2
                    ]

    one(0, False)

    def body(k1, carry):
        one(k1, True)
        return carry

    lax.fori_loop(1, NK, body, 0)

    def narrow(p, carry):
        at = pl.multiple_of(p * (4 * slab), 4 * slab)
        out_ref[pl.ds(at, 4 * slab), :] = wide_ref[pl.ds(at, 4 * slab), :].astype(BF)
        return carry

    lax.fori_loop(0, CH // 32, narrow, 0)


def pair_kernel(mask_ref, prev_ref, v_ref, next_ref, w_ref, tw_ref, table_ref, out_ref, sections, zhi, zlo, wide):
    group = pl.program_id(0)
    keep = mask_ref[0].astype(F32)

    def frames_of(n1, w):
        p2, v0, v1, v2, n0 = (
            frame_at(prev_ref, 0, n1),
            frame_at(v_ref, 0, n1),
            frame_at(v_ref, 1, n1),
            frame_at(v_ref, 2, n1),
            frame_at(next_ref, 0, n1),
        )
        return (
            w[0] * p2 + w[1] * v0 + w[2] * v1 + w[3] * v2,
            keep * (w[0] * v0 + w[1] * v1 + w[2] * v2) + w[3] * n0,
        )

    sections_of(frames_of, 2, w_ref, sections)
    for f in range(2):
        rows = pl.ds(pl.multiple_of(f * N2 + group * 16, 16), 16)
        first_half_bins(sections, tw_ref, zhi, zlo, f, rows)

    @pl.when(group == pl.num_programs(0) - 1)
    def _():
        emit_slabs(2, table_ref, zhi, zlo, wide, out_ref)


def single_kernel(
    mask_ref, prev_ref, v_ref, next_ref, side_ref, w_ref, tw_ref, table_ref, out_ref, sections, zhi, zlo, wide
):
    group = pl.program_id(0)
    keep = mask_ref[0].astype(F32)
    half = pl.num_programs(0) // 2

    @pl.when(group < half)
    def _():
        def frames_of(n1, w):
            return (
                w[0] * frame_at(side_ref, 0, n1)
                + w[1] * frame_at(prev_ref, 0, n1)
                + w[2] * frame_at(v_ref, 0, n1)
                + w[3] * frame_at(v_ref, 1, n1),
            )

        sections_of(frames_of, 1, w_ref, sections)

    @pl.when(group >= half)
    def _():
        def frames_of(n1, w):
            return (
                keep * (w[0] * frame_at(v_ref, 1, n1) + w[1] * frame_at(v_ref, 2, n1))
                + w[2] * frame_at(next_ref, 0, n1)
                + w[3] * frame_at(side_ref, 0, n1),
            )

        sections_of(frames_of, 1, w_ref, sections)

    first_half_bins(sections, tw_ref, zhi, zlo, 0, pl.ds(pl.multiple_of(group * 16, 16), 16))

    @pl.when(group == pl.num_programs(0) - 1)
    def _():
        emit_slabs(1, table_ref, zhi, zlo, wide, out_ref)


def spectra_call(body, n_out, mask, signal_arrays, window):
    signals = signal_arrays[0].shape[0]
    groups = signals // 16
    by_group = [pl.BlockSpec((16, x.shape[1]), lambda g: (g, 0)) for x in signal_arrays]
    whole = lambda shape: pl.BlockSpec(shape, lambda g: (0,) * len(shape))
    rows = CH * 2 * n_out
    return pl.pallas_call(
        body,
        out_shape=jax.ShapeDtypeStruct((rows, N2), BF),
        grid=(groups,),
        in_specs=[
            pl.BlockSpec(memory_space=pltpu.SMEM),
            *by_group,
            whole((TAPS, NFFT)),
            whole((NK, 2, N2)),
            whole((2 * N2, 2 * N2)),
        ],
        out_specs=whole((rows, N2)),
        scratch_shapes=[
            pltpu.VMEM((n_out, 8, 8, 16, N2), F32),
            pltpu.VMEM((NK, n_out * N2, 2 * N2), BF),
            pltpu.VMEM((NK, n_out * N2, 2 * N2), BF),
            pltpu.VMEM((rows, N2), F32),
        ],
        cost_estimate=pl.CostEstimate(flops=n_out * 10**10, transcendentals=0, bytes_accessed=n_out * 10**7),
        compiler_params=pltpu.CompilerParams(
            dimension_semantics=("arbitrary",), vmem_limit_bytes=56 * 1024 * 1024
        ),
    )(mask, *signal_arrays, window, jnp.asarray(twiddle_table()), jnp.asarray(bin_table()))


def correlate_kernel(own_ref, pair_ref, single_ref, out_ref, send_ref, wide, real, imag):
    ch = pl.program_id(0)
    own = own_ref[0]
    frames = 3 * N2
    scale = 1.0 / math.sqrt(frames)

    @pl.when(ch == 0)
    def _():
        first_lanes = lax.broadcasted_iota(jnp.int32, (16, N2), 1) < N2 // 2

        def body(t, carry):
            for src in range(2):
                for f in range(3):
                    ref, per, skip = (pair_ref, 32, f * 16) if f < 2 else (single_ref, 16, 0)
                    row = pl.multiple_of((t * 2 + src) * per + skip, 16)
                    tile = ref[pl.ds(row, 16), :].astype(F32)
                    if f == 2:
                        row = pl.multiple_of(((t + N2 - 1) % N2 * 2 + src) * per, 16)
                        tile = jnp.where(first_lanes, tile, ref[pl.ds(row, 16), :].astype(F32))
                    for part in range(2):
                        at = part * frames + f * N2 + t
                        wide[src, pl.ds(at, 8, stride=2 * frames), :] = tile[part * 8 : part * 8 + 8]
            return carry

        lax.fori_loop(0, N2, body, 0)

    at = pl.multiple_of(ch * 2 * frames, 2 * frames)
    rows = pl.ds(at, 2 * frames)
    both = jnp.concatenate([wide[0, rows, :].astype(BF), wide[1, rows, :].astype(BF)], axis=1)
    xr, xi = both[:frames], both[frames:]
    dims = (((0,), (0,)), ((), ()))
    r = lax.dot_general(both, both, dims, preferred_element_type=F32) * scale
    p = lax.dot_general(xi, xr, dims, preferred_element_type=F32) * scale
    real[...] = r
    imag[...] = p - p.T
    mine = pl.ds(pl.multiple_of(own * N2, N2), N2)
    theirs = pl.ds(pl.multiple_of((1 - own) * N2, N2), N2)
    out_ref[0, :, : 2 * N2] = real[mine, :]
    out_ref[0, :, 2 * N2 :] = imag[mine, :]
    rows_r, rows_i = real[theirs, :], imag[theirs, :]
    first = own == 0
    cross_r = jnp.where(first, rows_r[:, :N2], rows_r[:, N2:])
    cross_i = jnp.where(first, rows_i[:, :N2], rows_i[:, N2:])
    diag_r = jnp.where(first, rows_r[:, N2:], rows_r[:, :N2])
    diag_i = jnp.where(first, rows_i[:, N2:], rows_i[:, :N2])
    upper = lax.broadcasted_iota(jnp.int32, (N2, N2), 0) <= lax.broadcasted_iota(jnp.int32, (N2, N2), 1)
    send_ref[0, :, :N2] = cross_r.astype(BF)
    send_ref[0, :, N2 : 2 * N2] = cross_i.astype(BF)
    send_ref[0, :, 2 * N2 :] = jnp.where(upper, diag_r, diag_i).astype(BF)


def correlate(own, pair, single):
    frames = 3 * N2
    grid_spec = pltpu.PrefetchScalarGridSpec(
        num_scalar_prefetch=1,
        grid=(8,),
        in_specs=[
            pl.BlockSpec(pair.shape, lambda c, own: (0, 0)),
            pl.BlockSpec(single.shape, lambda c, own: (0, 0)),
        ],
        out_specs=[
            pl.BlockSpec((1, N2, 4 * N2), lambda c, own: (own[0] * 8 + c, 0, 0)),
            pl.BlockSpec((1, N2, 3 * N2), lambda c, own: (c, 0, 0)),
        ],
        scratch_shapes=[
            pltpu.VMEM((2, 8 * 2 * frames, N2), F32),
            pltpu.VMEM((2 * N2, 2 * N2), F32),
            pltpu.VMEM((2 * N2, 2 * N2), F32),
        ],
    )
    return pl.pallas_call(
        correlate_kernel,
        out_shape=[
            jax.ShapeDtypeStruct((16, N2, 4 * N2), F32),
            jax.ShapeDtypeStruct((8, N2, 3 * N2), BF),
        ],
        grid_spec=grid_spec,
        cost_estimate=pl.CostEstimate(flops=10**10, transcendentals=0, bytes_accessed=10**7),
        compiler_params=pltpu.CompilerParams(
            dimension_semantics=("arbitrary",), vmem_limit_bytes=40 * 1024 * 1024
        ),
    )(own, pair, single)


def finish_kernel(own_ref, part_ref, got_ref, out_ref):
    first = own_ref[0] == 0
    cross_r = got_ref[0, :, :N2].astype(F32)
    cross_i = got_ref[0, :, N2 : 2 * N2].astype(F32)
    packed = got_ref[0, :, 2 * N2 :].astype(F32)
    flipped = packed.T
    row = lax.broadcasted_iota(jnp.int32, (N2, N2), 0)
    col = lax.broadcasted_iota(jnp.int32, (N2, N2), 1)
    diag_r = jnp.where(row <= col, packed, flipped)
    diag_i = jnp.where(row > col, packed, jnp.where(row < col, -flipped, 0.0))
    out_ref[0, :, :N2] = jnp.where(first, diag_r, cross_r)
    out_ref[0, :, N2 : 2 * N2] = jnp.where(first, cross_r, diag_r)
    out_ref[0, :, 2 * N2 : 3 * N2] = jnp.where(first, diag_i, cross_i)
    out_ref[0, :, 3 * N2 :] = jnp.where(first, cross_i, diag_i)


def finish(own, part, got):
    grid_spec = pltpu.PrefetchScalarGridSpec(
        num_scalar_prefetch=1,
        grid=(8,),
        in_specs=[
            pl.BlockSpec(memory_space=pl.ANY),
            pl.BlockSpec((1, N2, 3 * N2), lambda c, own: (c, 0, 0)),
        ],
        out_specs=pl.BlockSpec((1, N2, 4 * N2), lambda c, own: ((1 - own[0]) * 8 + c, 0, 0)),
    )
    return pl.pallas_call(
        finish_kernel,
        out_shape=jax.ShapeDtypeStruct(part.shape, F32),
        grid_spec=grid_spec,
        input_output_aliases={1: 0},
        compiler_params=pltpu.CompilerParams(dimension_semantics=("arbitrary",)),
    )(own, part, got)


def per_device(voltages, pfb_window):
    signals = voltages.shape[0]
    peers = lax.axis_size("ta")
    half = signals // 2
    to_right = [(i, i + 1) for i in range(peers - 1)]
    to_left = [(i, (i - 1) % peers) for i in range(peers)]
    inner = (lax.axis_index("ta") < peers - 1).astype(jnp.int32).reshape(1)
    own = lax.axis_index("aa").astype(jnp.int32).reshape(1)
    prev = lax.ppermute(voltages[:, 2 * NFFT :], "ta", to_right)
    following = lax.ppermute(voltages[:, :NFFT], "ta", to_left)
    prev_side = lax.ppermute(voltages[:half, NFFT : 2 * NFFT], "ta", to_right)
    next_side = lax.ppermute(voltages[half:, NFFT : 2 * NFFT], "ta", to_left)
    pair = spectra_call(pair_kernel, 2, inner, (prev, voltages, following), pfb_window)
    pair = lax.all_to_all(pair, ("ta", "aa"), split_axis=0, concat_axis=0, tiled=True)
    side = jnp.concatenate([prev_side, next_side], axis=0)
    single = spectra_call(single_kernel, 1, inner, (prev, voltages, following, side), pfb_window)
    single = lax.all_to_all(single, ("ta", "aa"), split_axis=0, concat_axis=0, tiled=True)
    part, send = correlate(own, pair, single)
    got = lax.ppermute(send, "aa", [(0, 1), (1, 0)])
    return finish(own, part, got)


def solution(mesh):
    return jax.shard_map(
        per_device,
        mesh=mesh,
        in_specs=(P("aa", "ta"), P()),
        out_specs=P("ta", "aa", None),
        check_vma=False,
    )
```

```python
import math

import jax
import jax.numpy as jnp
import numpy as np
from jax import lax
from jax.experimental import pallas as pl
from jax.experimental.pallas import tpu as pltpu
from jax.sharding import PartitionSpec as P

NFFT = 8192
CH = 2048
TAPS = 4
CH_OFF = 1024
N1 = 64
N2 = 128
NK = 33
NJ = CH // N1
K2 = CH_OFF // N1
HALF = math.sqrt(0.5)
BF = jnp.bfloat16
F32 = jnp.float32


def twiddle_table():
    phase = np.outer(np.arange(NK), np.arange(N2)) * (2.0 * np.pi / NFFT)
    return np.stack([np.cos(phase), np.sin(phase)], axis=1).astype(np.float32)


def bin_table():
    scale = 1.0 / math.sqrt(NFFT)
    bins = np.arange(K2, K2 + NJ)
    rows = []
    for bin_set, sign in ((bins, 1.0), (-(bins + 1), -1.0)):
        phase = np.outer(bin_set, np.arange(N2)) % N2 * (2.0 * np.pi / N2)
        cosine, sine = np.cos(phase) * scale, np.sin(phase) * scale
        rows.append(np.concatenate([cosine, sine], axis=1))
        rows.append(sign * np.concatenate([-sine, cosine], axis=1))
    table = np.concatenate(rows, axis=0)
    high = table.astype(BF)
    low = (table - high.astype(np.float64)).astype(BF)
    return np.concatenate([high, low], axis=0)


def real_dft8(x):
    s0, d0 = x[0] + x[4], x[0] - x[4]
    s1, d1 = x[1] + x[5], x[1] - x[5]
    s2, d2 = x[2] + x[6], x[2] - x[6]
    s3, d3 = x[3] + x[7], x[3] - x[7]
    e0, e1 = s0 + s2, s1 + s3
    u, v = HALF * (d1 - d3), HALF * (d1 + d3)
    return [(e0 + e1, None), (d0 + u, -(d2 + v)), (s0 - s2, s3 - s1), (d0 - u, d2 - v), (e0 - e1, None)]


def complex_dft8(z, first_half=False):
    sr = [z[j][0] + z[j + 4][0] for j in range(4)]
    si = [z[j][1] + z[j + 4][1] for j in range(4)]
    dr = [z[j][0] - z[j + 4][0] for j in range(4)]
    di = [z[j][1] - z[j + 4][1] for j in range(4)]
    out = [None] * 8
    pr, pi = dr[1], di[1]
    dr[1], di[1] = HALF * (pr + pi), HALF * (pi - pr)
    dr[2], di[2] = di[2], -dr[2]
    pr, pi = dr[3], di[3]
    dr[3], di[3] = HALF * (pi - pr), -HALF * (pr + pi)
    for base, (ar, ai) in ((0, (sr, si)), (1, (dr, di))):
        er, ei = ar[0] + ar[2], ai[0] + ai[2]
        fr, fi = ar[1] + ar[3], ai[1] + ai[3]
        gr, gi = ar[0] - ar[2], ai[0] - ai[2]
        hr, hi = ar[1] - ar[3], ai[1] - ai[3]
        out[base] = (er + fr, ei + fi)
        out[base + 2] = (gr + hi, gi - hr)
        if not first_half:
            out[base + 4] = (er - fr, ei - fi)
            out[base + 6] = (gr - hi, gi + hr)
    return out


def first_half_bins(sections, tw_ref, zhi_ref, zlo_ref, frame, rows):
    def keep(k1, re, im, conj):
        c, s = tw_ref[k1, 0:1, :], tw_ref[k1, 1:2, :]
        if im is None:
            zr, zi = re * c, -(re * s)
        elif conj:
            zr, zi = re * c - im * s, -(im * c + re * s)
        else:
            zr, zi = re * c + im * s, im * c - re * s
        for part, z in ((0, zr), (1, zi)):
            high = z.astype(BF)
            low = (z - high.astype(F32)).astype(BF)
            zhi_ref[k1, rows, part * N2 : (part + 1) * N2] = high
            zlo_ref[k1, rows, part * N2 : (part + 1) * N2] = low

    spectrum = real_dft8([sections[frame, 0, b] for b in range(8)])
    for r in range(5):
        keep(8 * r, spectrum[r][0], spectrum[r][1], False)
    for q in (1, 2, 3):
        z = []
        for b in range(8):
            re, im = sections[frame, 2 * q - 1, b], sections[frame, 2 * q, b]
            if b:
                c, s = math.cos(2 * math.pi * b * q / N1), math.sin(2 * math.pi * b * q / N1)
                re, im = re * c + im * s, im * c - re * s
            z.append((re, im))
        for r, (re, im) in enumerate(complex_dft8(z)):
            k1 = q + 8 * r
            if k1 <= 32:
                keep(k1, re, im, False)
            else:
                keep(N1 - k1, re, im, True)
    z = []
    for b in range(8):
        x = sections[frame, 7, b]
        c, s = math.cos(2 * math.pi * b * 4 / N1), math.sin(2 * math.pi * b * 4 / N1)
        z.append((x * c, x * -s) if b else (x, jnp.zeros_like(x)))
    out = complex_dft8(z, first_half=True)
    for r in range(4):
        keep(4 + 8 * r, out[r][0], out[r][1], False)


def sections_of(frames_of, n_out, w_ref, sections):
    for b in range(8):
        filtered = [[] for _ in range(n_out)]
        for a in range(8):
            n1 = 8 * a + b
            w = [w_ref[k : k + 1, n1 * N2 : (n1 + 1) * N2] for k in range(TAPS)]
            for f, value in enumerate(frames_of(n1, w)):
                filtered[f].append(value)
        for f in range(n_out):
            spectrum = real_dft8(filtered[f])
            sections[f, 0, b] = spectrum[0][0]
            for q in (1, 2, 3):
                sections[f, 2 * q - 1, b] = spectrum[q][0]
                sections[f, 2 * q, b] = spectrum[q][1]
            sections[f, 7, b] = spectrum[4][0]


def emit_slabs(n_out, table_ref, zhi_ref, zlo_ref, wide_ref, slabs_ref, out_ref, out_sems):
    slab = n_out * 16
    block = 8 * slab
    lap = block + 1

    def one(k1, mirror):
        dims = (((1,), (1,)), ((), ()))
        both = lax.dot_general(table_ref[...], zhi_ref[k1], dims, preferred_element_type=F32)
        more = lax.dot_general(table_ref[0:N2, :], zlo_ref[k1], dims, preferred_element_type=F32)
        spectrum = both[:N2] + both[N2:] + more
        for side in range(2 if mirror else 1):
            ch = N1 - k1 if side else k1
            start = (ch // 8) * slab + ch % 8
            for part in range(2):
                at = (side * 2 + part) * NJ
                for f in range(n_out):
                    wide_ref[pl.ds(start + (f * 2 + part) * 8, NJ, stride=lap), :] = spectrum[
                        at : at + NJ, f * N2 : (f + 1) * N2
                    ]

    one(0, False)

    def body(k1, carry):
        one(k1, True)
        return carry

    lax.fori_loop(1, NK, body, 0)

    def copy_out(j):
        rows = pl.ds(pl.multiple_of(j * block, block), block)
        return pltpu.make_async_copy(slabs_ref.at[rows], out_ref.at[rows], out_sems.at[j])

    def narrow(j, carry):
        slabs_ref[pl.ds(pl.multiple_of(j * block, block), block), :] = wide_ref[pl.ds(j * lap, block), :].astype(BF)
        copy_out(j).start()
        return carry

    lax.fori_loop(0, NJ, narrow, 0)

    def drain(j, carry):
        copy_out(j).wait()
        return carry

    lax.fori_loop(0, NJ, drain, 0)


def fft_kernel(n_out, n_parts, slots, taps_a, taps_b, mask_ref, v_hbm, *refs):
    parts, refs = refs[:n_parts], refs[n_parts:]
    w_ref, tw_ref, table_ref, out_ref, v_buf, hist_buf, sections, zhi, zlo, wide, slabs, sems, out_sems = refs
    keep = mask_ref[0].astype(F32)
    groups = v_buf.shape[0] // 16

    def copies(g, side):
        rows = pl.ds(pl.multiple_of(g * 16, 16), 16)
        jobs = [pltpu.make_async_copy(v_hbm.at[rows], v_buf.at[rows], sems.at[0, g])]
        for k, slot in enumerate(slots):
            part, skip = slot[side]
            source = parts[part].at[pl.ds(pl.multiple_of((g + skip) * 16, 16), 16)]
            jobs.append(pltpu.make_async_copy(source, hist_buf.at[k, rows], sems.at[k + 1, g]))
        return jobs

    for g in range(groups):
        for job in copies(g, g // (groups // 2)):
            job.start()

    def run(taps, side):
        def body(g, carry):
            for job in copies(g, side):
                job.wait()
            rows = pl.ds(pl.multiple_of(g * 16, 16), 16)

            def frames_of(n1, w):
                lanes = slice(n1 * N2, (n1 + 1) * N2)
                v = [v_buf[rows, i * NFFT + n1 * N2 : i * NFFT + (n1 + 1) * N2].astype(F32) for i in range(3)]
                h = [hist_buf[k, rows, lanes].astype(F32) for k in range(len(slots))]
                return taps(keep, w, v, h)

            sections_of(frames_of, n_out, w_ref, sections)
            for f in range(n_out):
                at = pl.multiple_of(f * N2 + g * 16, 16)
                first_half_bins(sections, tw_ref, zhi, zlo, f, pl.ds(at, 16))
            return carry

        return body

    lax.fori_loop(0, groups // 2, run(taps_a, 0), 0)
    lax.fori_loop(groups // 2, groups, run(taps_b, 1), 0)
    emit_slabs(n_out, table_ref, zhi, zlo, wide, slabs, out_ref, out_sems)


def first_a(keep, w, v, h):
    return (w[0] * h[0] + w[1] * v[0] + w[2] * v[1] + w[3] * v[2],)


def first_b(keep, w, v, h):
    return (keep * (w[0] * v[0] + w[1] * v[1] + w[2] * v[2]) + w[3] * h[0],)


def second_a(keep, w, v, h):
    near, one_off, two_off = h
    return (
        keep * (w[0] * v[0] + w[1] * v[1] + w[2] * v[2]) + w[3] * one_off,
        w[0] * two_off + w[1] * near + w[2] * v[0] + w[3] * v[1],
    )


def second_b(keep, w, v, h):
    near, one_off, two_off = h
    return (
        w[0] * one_off + w[1] * v[0] + w[2] * v[1] + w[3] * v[2],
        keep * (w[0] * v[1] + w[1] * v[2]) + w[2] * near + w[3] * two_off,
    )


def spectra_call(n_out, taps_a, taps_b, mask, voltages, parts, slots, window):
    signals = voltages.shape[0]
    n_hist = len(slots)
    rows = CH * 2 * n_out
    vmem = pl.BlockSpec(memory_space=pltpu.VMEM)
    hbm = pl.BlockSpec(memory_space=pltpu.HBM)
    return pl.pallas_call(
        lambda *refs: fft_kernel(n_out, len(parts), slots, taps_a, taps_b, *refs),
        out_shape=jax.ShapeDtypeStruct((rows, N2), BF),
        in_specs=[pl.BlockSpec(memory_space=pltpu.SMEM), hbm] + [hbm] * len(parts) + [vmem] * 3,
        out_specs=hbm,
        scratch_shapes=[
            pltpu.VMEM(voltages.shape, BF),
            pltpu.VMEM((n_hist, signals, NFFT), BF),
            pltpu.VMEM((n_out, 8, 8, 16, N2), F32),
            pltpu.VMEM((NK, n_out * N2, 2 * N2), BF),
            pltpu.VMEM((NK, n_out * N2, 2 * N2), BF),
            pltpu.VMEM((rows + NJ, N2), F32),
            pltpu.VMEM((rows, N2), BF),
            pltpu.SemaphoreType.DMA((n_hist + 1, signals // 16)),
            pltpu.SemaphoreType.DMA((NJ,)),
        ],
        cost_estimate=pl.CostEstimate(flops=n_out * 10**10, transcendentals=0, bytes_accessed=n_out * 10**7),
        compiler_params=pltpu.CompilerParams(vmem_limit_bytes=56 * 1024 * 1024),
    )(mask, voltages, *parts, window, jnp.asarray(twiddle_table()), jnp.asarray(bin_table()))


LAP = 2 * N2 + 1


def spread_kernel(in_ref, out_ref, wide):
    def body(t, carry):
        for src in range(2):
            tile = in_ref[pl.ds(pl.multiple_of((t * 2 + src) * 16, 16), 16), :].astype(F32)
            for part in range(2):
                wide[src, pl.ds(part * N2 + t, 8, stride=LAP), :] = tile[part * 8 : part * 8 + 8]
        return carry

    lax.fori_loop(0, N2, body, 0)
    for ch in range(8):
        for src in range(2):
            out_ref[ch, :, src * N2 : (src + 1) * N2] = wide[src, ch * LAP : ch * LAP + 2 * N2, :].astype(BF)


def spread(first):
    vmem = pl.BlockSpec(memory_space=pltpu.VMEM)
    return pl.pallas_call(
        spread_kernel,
        out_shape=jax.ShapeDtypeStruct((8, 2 * N2, 2 * N2), BF),
        in_specs=[vmem],
        out_specs=vmem,
        scratch_shapes=[pltpu.VMEM((2, 8 * LAP + 8, N2), F32)],
        cost_estimate=pl.CostEstimate(flops=2 * 10**9, transcendentals=0, bytes_accessed=10**6),
        compiler_params=pltpu.CompilerParams(vmem_limit_bytes=16 * 1024 * 1024),
    )(first)


def correlate_kernel(own_ref, first_ref, second_ref, out_hbm, send_ref, wide, real, imag, rows_buf, sems):
    own = own_ref[0]
    scale = 1.0 / math.sqrt(3 * N2)
    first_lanes = lax.broadcasted_iota(jnp.int32, (16, N2), 1) < N2 // 2

    def body(t, carry):
        for src in range(2):
            for f in range(2):
                row = pl.multiple_of((t * 2 + src) * 32 + f * 16, 16)
                tile = second_ref[pl.ds(row, 16), :].astype(F32)
                if f:
                    row = pl.multiple_of(((t + N2 - 1) % N2 * 2 + src) * 32 + 16, 16)
                    tile = jnp.where(first_lanes, tile, second_ref[pl.ds(row, 16), :].astype(F32))
                for part in range(2):
                    wide[f, src, pl.ds(part * N2 + t, 8, stride=LAP), :] = tile[part * 8 : part * 8 + 8]
        return carry

    lax.fori_loop(0, N2, body, 0)

    first = own == 0
    mine = pl.ds(pl.multiple_of(own * N2, N2), N2)
    theirs = pl.ds(pl.multiple_of((1 - own) * N2, N2), N2)
    upper = lax.broadcasted_iota(jnp.int32, (N2, N2), 0) <= lax.broadcasted_iota(jnp.int32, (N2, N2), 1)
    half_lanes = lax.broadcasted_iota(jnp.int32, (2 * N2, 2 * N2), 1) % N2 < N2 // 2
    dims = (((0,), (0,)), ((), ()))

    def copy_out(ch):
        return pltpu.make_async_copy(rows_buf.at[ch], out_hbm.at[own * 8 + ch], sems.at[ch])

    for ch in range(8):
        rows = slice(ch * LAP, ch * LAP + 2 * N2)
        g1, g2 = (
            jnp.concatenate([wide[f, 0, rows, :].astype(BF), wide[f, 1, rows, :].astype(BF)], axis=1)
            for f in range(2)
        )
        g0 = first_ref[ch]
        x = [jnp.where(half_lanes, g0, g1), jnp.where(half_lanes, g1, g0), g2]
        xr = jnp.concatenate([part[:N2] for part in x], axis=0)
        xi = jnp.concatenate([part[N2:] for part in x], axis=0)
        both = jnp.concatenate([xr, xi], axis=0)
        p = lax.dot_general(xi, xr, dims, preferred_element_type=F32) * scale
        real[...] = lax.dot_general(both, both, dims, preferred_element_type=F32) * scale
        imag[...] = p - p.T
        rows_buf[ch, :, : 2 * N2] = real[mine, :]
        rows_buf[ch, :, 2 * N2 :] = imag[mine, :]
        copy_out(ch).start()
        rows_r, rows_i = real[theirs, :], imag[theirs, :]
        cross_r = jnp.where(first, rows_r[:, :N2], rows_r[:, N2:])
        cross_i = jnp.where(first, rows_i[:, :N2], rows_i[:, N2:])
        diag_r = jnp.where(first, rows_r[:, N2:], rows_r[:, :N2])
        diag_i = jnp.where(first, rows_i[:, N2:], rows_i[:, :N2])
        send_ref[ch, :, :N2] = cross_r.astype(BF)
        send_ref[ch, :, N2 : 2 * N2] = cross_i.astype(BF)
        send_ref[ch, :, 2 * N2 :] = jnp.where(upper, diag_r, diag_i).astype(BF)

    for ch in range(8):
        copy_out(ch).wait()


def correlate(own, first, second):
    vmem = pl.BlockSpec(memory_space=pltpu.VMEM)
    return pl.pallas_call(
        correlate_kernel,
        out_shape=[
            jax.ShapeDtypeStruct((16, N2, 4 * N2), F32),
            jax.ShapeDtypeStruct((8, N2, 3 * N2), BF),
        ],
        in_specs=[pl.BlockSpec(memory_space=pltpu.SMEM), vmem, vmem],
        out_specs=[pl.BlockSpec(memory_space=pltpu.HBM), vmem],
        scratch_shapes=[
            pltpu.VMEM((2, 2, 8 * LAP + 8, N2), F32),
            pltpu.VMEM((2 * N2, 2 * N2), F32),
            pltpu.VMEM((2 * N2, 2 * N2), F32),
            pltpu.VMEM((8, N2, 4 * N2), F32),
            pltpu.SemaphoreType.DMA((8,)),
        ],
        cost_estimate=pl.CostEstimate(flops=5 * 10**9, transcendentals=0, bytes_accessed=10**7),
        compiler_params=pltpu.CompilerParams(vmem_limit_bytes=40 * 1024 * 1024),
    )(own, first, second)


def finish_kernel(own_ref, part_ref, got_ref, out_hbm, rows_buf, sems):
    own = own_ref[0]
    first = own == 0
    row = lax.broadcasted_iota(jnp.int32, (N2, N2), 0)
    col = lax.broadcasted_iota(jnp.int32, (N2, N2), 1)

    def copy_out(ch):
        return pltpu.make_async_copy(rows_buf.at[ch], out_hbm.at[(1 - own) * 8 + ch], sems.at[ch])

    for ch in range(8):
        cross_r = got_ref[ch, :, :N2].astype(F32)
        cross_i = got_ref[ch, :, N2 : 2 * N2].astype(F32)
        packed = got_ref[ch, :, 2 * N2 :].astype(F32)
        flipped = packed.T
        diag_r = jnp.where(row <= col, packed, flipped)
        diag_i = jnp.where(row > col, packed, jnp.where(row < col, -flipped, 0.0))
        rows_buf[ch, :, :N2] = jnp.where(first, diag_r, cross_r)
        rows_buf[ch, :, N2 : 2 * N2] = jnp.where(first, cross_r, diag_r)
        rows_buf[ch, :, 2 * N2 : 3 * N2] = jnp.where(first, diag_i, cross_i)
        rows_buf[ch, :, 3 * N2 :] = jnp.where(first, cross_i, diag_i)
        copy_out(ch).start()
    for ch in range(8):
        copy_out(ch).wait()


def finish(own, part, got):
    return pl.pallas_call(
        finish_kernel,
        out_shape=jax.ShapeDtypeStruct(part.shape, F32),
        in_specs=[
            pl.BlockSpec(memory_space=pltpu.SMEM),
            pl.BlockSpec(memory_space=pltpu.HBM),
            pl.BlockSpec(memory_space=pltpu.VMEM),
        ],
        out_specs=pl.BlockSpec(memory_space=pltpu.HBM),
        scratch_shapes=[pltpu.VMEM((8, N2, 4 * N2), F32), pltpu.SemaphoreType.DMA((8,))],
        input_output_aliases={1: 0},
        compiler_params=pltpu.CompilerParams(vmem_limit_bytes=8 * 1024 * 1024),
    )(own, part, got)


def cut_kernel(plan, v_hbm, *refs):
    outs, sems = refs[: len(plan)], refs[len(plan)]
    jobs = []
    for out, pieces in zip(outs, plan):
        at = 0
        for (start, stop), frame in pieces:
            for row in range(start, stop, 16):
                source = v_hbm.at[pl.ds(row, 16), pl.ds(frame * NFFT, NFFT)]
                jobs.append(pltpu.make_async_copy(source, out.at[pl.ds(at, 16)], sems.at[len(jobs)]))
                at += 16
    for job in jobs:
        job.start()
    for job in jobs:
        job.wait()


def cut(voltages, plan):
    sizes = [sum(stop - start for (start, stop), _ in pieces) for pieces in plan]
    hbm = pl.BlockSpec(memory_space=pltpu.HBM)
    return pl.pallas_call(
        lambda *refs: cut_kernel(plan, *refs),
        out_shape=[jax.ShapeDtypeStruct((size, NFFT), BF) for size in sizes],
        in_specs=[hbm],
        out_specs=[pl.BlockSpec(memory_space=pltpu.VMEM)] * len(plan),
        scratch_shapes=[pltpu.SemaphoreType.DMA((sum(sizes) // 16,))],
        cost_estimate=pl.CostEstimate(flops=10**9, transcendentals=0, bytes_accessed=10**7),
        compiler_params=pltpu.CompilerParams(vmem_limit_bytes=60 * 1024 * 1024),
    )(voltages)


def per_device(voltages, pfb_window):
    signals = voltages.shape[0]
    peers = lax.axis_size("ta")
    half = signals // 2
    to_right = [(i, i + 1) for i in range(peers - 1)]
    to_left = [(i, (i - 1) % peers) for i in range(peers)]
    inner = (lax.axis_index("ta") < peers - 1).astype(jnp.int32).reshape(1)
    own = lax.axis_index("aa").astype(jnp.int32).reshape(1)
    to_r, to_l = cut(voltages, ((((0, half), 2),), (((half, signals), 0),)))
    prev_a = lax.ppermute(to_r, "ta", to_right)
    next_b = lax.ppermute(to_l, "ta", to_left)
    top, bottom = (0, half), (half, signals)
    to_r, to_l = cut(voltages, (((top, 1), (bottom, 2)), ((top, 0), (bottom, 1))))
    right = lax.ppermute(to_r, "ta", to_right)
    left = lax.ppermute(to_l, "ta", to_left)
    low = -(half // 16)
    near = ((0, 0), (1, low))
    first = spectra_call(1, first_a, first_b, inner, voltages, (prev_a, next_b), (near,), pfb_window)
    first = lax.all_to_all(first, ("ta", "aa"), split_axis=0, concat_axis=0, tiled=True)
    slots = (near, ((2, 0), (3, 0)), ((3, 0), (2, 0)))
    parts = (prev_a, next_b, left, right)
    second = spectra_call(2, second_a, second_b, inner, voltages, parts, slots, pfb_window)
    second = lax.all_to_all(second, ("ta", "aa"), split_axis=0, concat_axis=0, tiled=True)
    first = spread(first)
    part, send = correlate(own, first, second)
    got = lax.ppermute(send, "aa", [(0, 1), (1, 0)])
    return finish(own, part, got)


def solution(mesh):
    return jax.shard_map(
        per_device,
        mesh=mesh,
        in_specs=(P("aa", "ta"), P()),
        out_specs=P("ta", "aa", None),
        check_vma=False,
    )
```

```python
import math

import jax
import jax.numpy as jnp
import numpy as np
from jax import lax
from jax.experimental import pallas as pl
from jax.experimental.pallas import tpu as pltpu
from jax.sharding import PartitionSpec as P

NFFT = 8192
CH = 2048
TAPS = 4
CH_OFF = 1024
N1 = 64
N2 = 128
NK = 33
NJ = CH // N1
K2 = CH_OFF // N1
HALF = math.sqrt(0.5)
UNROLL = 32
BF = jnp.bfloat16
F32 = jnp.float32


def twiddle_table():
    phase = np.outer(np.arange(NK), np.arange(N2)) * (2.0 * np.pi / NFFT)
    return np.stack([np.cos(phase), np.sin(phase)], axis=1).astype(np.float32)


def bin_table():
    scale = 1.0 / math.sqrt(NFFT)
    bins = np.arange(K2, K2 + NJ)
    rows = []
    for bin_set, sign in ((bins, 1.0), (-(bins + 1), -1.0)):
        phase = np.outer(bin_set, np.arange(N2)) % N2 * (2.0 * np.pi / N2)
        cosine, sine = np.cos(phase) * scale, np.sin(phase) * scale
        rows.append(np.concatenate([cosine, sine], axis=1))
        rows.append(sign * np.concatenate([-sine, cosine], axis=1))
    table = np.concatenate(rows, axis=0)
    high = table.astype(BF)
    low = (table - high.astype(np.float64)).astype(BF)
    return np.concatenate([high, low], axis=0).T


def real_dft8(x):
    s0, d0 = x[0] + x[4], x[0] - x[4]
    s1, d1 = x[1] + x[5], x[1] - x[5]
    s2, d2 = x[2] + x[6], x[2] - x[6]
    s3, d3 = x[3] + x[7], x[3] - x[7]
    e0, e1 = s0 + s2, s1 + s3
    u, v = HALF * (d1 - d3), HALF * (d1 + d3)
    return [(e0 + e1, None), (d0 + u, -(d2 + v)), (s0 - s2, s3 - s1), (d0 - u, d2 - v), (e0 - e1, None)]


def complex_dft8(z, first_half=False):
    sr = [z[j][0] + z[j + 4][0] for j in range(4)]
    si = [z[j][1] + z[j + 4][1] for j in range(4)]
    dr = [z[j][0] - z[j + 4][0] for j in range(4)]
    di = [z[j][1] - z[j + 4][1] for j in range(4)]
    out = [None] * 8
    pr, pi = dr[1], di[1]
    dr[1], di[1] = HALF * (pr + pi), HALF * (pi - pr)
    dr[2], di[2] = di[2], -dr[2]
    pr, pi = dr[3], di[3]
    dr[3], di[3] = HALF * (pi - pr), -HALF * (pr + pi)
    for base, (ar, ai) in ((0, (sr, si)), (1, (dr, di))):
        er, ei = ar[0] + ar[2], ai[0] + ai[2]
        fr, fi = ar[1] + ar[3], ai[1] + ai[3]
        gr, gi = ar[0] - ar[2], ai[0] - ai[2]
        hr, hi = ar[1] - ar[3], ai[1] - ai[3]
        out[base] = (er + fr, ei + fi)
        out[base + 2] = (gr + hi, gi - hr)
        if not first_half:
            out[base + 4] = (er - fr, ei - fi)
            out[base + 6] = (gr - hi, gi + hr)
    return out


def first_half_bins(sections, tw_ref, z_ref, frame, row):
    low_row = row + z_ref.shape[1] // 2

    def keep(k1, re, im, conj):
        c, s = tw_ref[k1, 0:1, :], tw_ref[k1, 1:2, :]
        if im is None:
            zr, zi = re * c, -(re * s)
        elif conj:
            zr, zi = re * c - im * s, -(im * c + re * s)
        else:
            zr, zi = re * c + im * s, im * c - re * s
        for part, z in ((0, zr), (1, zi)):
            high = z.astype(BF)
            low = (z - high.astype(F32)).astype(BF)
            lanes = slice(part * N2, (part + 1) * N2)
            z_ref[k1, pl.ds(pl.multiple_of(row, 16), 16), lanes] = high
            z_ref[k1, pl.ds(pl.multiple_of(low_row, 16), 16), lanes] = low

    spectrum = real_dft8([sections[frame, 0, b] for b in range(8)])
    for r in range(5):
        keep(8 * r, spectrum[r][0], spectrum[r][1], False)
    for q in (1, 2, 3):
        z = []
        for b in range(8):
            re, im = sections[frame, 2 * q - 1, b], sections[frame, 2 * q, b]
            if b:
                c, s = math.cos(2 * math.pi * b * q / N1), math.sin(2 * math.pi * b * q / N1)
                re, im = re * c + im * s, im * c - re * s
            z.append((re, im))
        for r, (re, im) in enumerate(complex_dft8(z)):
            k1 = q + 8 * r
            if k1 <= 32:
                keep(k1, re, im, False)
            else:
                keep(N1 - k1, re, im, True)
    z = []
    for b in range(8):
        x = sections[frame, 7, b]
        c, s = math.cos(2 * math.pi * b * 4 / N1), math.sin(2 * math.pi * b * 4 / N1)
        z.append((x * c, x * -s) if b else (x, jnp.zeros_like(x)))
    out = complex_dft8(z, first_half=True)
    for r in range(4):
        keep(4 + 8 * r, out[r][0], out[r][1], False)


def sections_of(frames_of, n_out, w_ref, sections):
    for b in range(8):
        filtered = [[] for _ in range(n_out)]
        for a in range(8):
            n1 = 8 * a + b
            w = [w_ref[k : k + 1, n1 * N2 : (n1 + 1) * N2] for k in range(TAPS)]
            for f, value in enumerate(frames_of(n1, w)):
                filtered[f].append(value)
        for f in range(n_out):
            spectrum = real_dft8(filtered[f])
            sections[f, 0, b] = spectrum[0][0]
            for q in (1, 2, 3):
                sections[f, 2 * q - 1, b] = spectrum[q][0]
                sections[f, 2 * q, b] = spectrum[q][1]
            sections[f, 7, b] = spectrum[4][0]


def emit_slabs(n_out, table_ref, z_ref, wide_ref, slabs_ref, out_ref, out_sems):
    slab = n_out * 16
    block = 8 * slab
    lap = block + 1
    rows = n_out * N2

    def some(first, count, mirror):
        left = z_ref[pl.ds(first, count)].reshape(count * 2 * rows, 2 * N2)
        product = jnp.dot(left, table_ref[...], preferred_element_type=F32)
        for u in range(count):
            k1 = first + u
            high, low = (product[(2 * u + i) * rows : (2 * u + i + 1) * rows] for i in range(2))
            spectrum = high[:, :N2] + high[:, N2:] + low[:, :N2]
            for f in range(n_out):
                flipped = spectrum[f * N2 : (f + 1) * N2].T
                for side in range(2 if mirror else 1):
                    ch = N1 - k1 if side else k1
                    start = (ch >> 3) * slab + (ch & 7) + f * 16
                    for part in range(2):
                        at = (side * 2 + part) * NJ
                        wide_ref[pl.ds(start + part * 8, NJ, stride=lap), :] = flipped[at : at + NJ]

    some(0, 1, False)
    lax.fori_loop(0, (NK - 1) // UNROLL, lambda i, c: (some(1 + i * UNROLL, UNROLL, True), c)[1], 0)

    def copy_out(j):
        rows = pl.ds(pl.multiple_of(j * block, block), block)
        return pltpu.make_async_copy(slabs_ref.at[rows], out_ref.at[rows], out_sems.at[j])

    def narrow(j, carry):
        slabs_ref[pl.ds(pl.multiple_of(j * block, block), block), :] = wide_ref[pl.ds(j * lap, block), :].astype(BF)
        copy_out(j).start()
        return carry

    lax.fori_loop(0, NJ, narrow, 0)

    def drain(j, carry):
        copy_out(j).wait()
        return carry

    lax.fori_loop(0, NJ, drain, 0)


def fft_kernel(n_out, n_parts, slots, taps_a, taps_b, mask_ref, v_hbm, *refs):
    parts, refs = refs[:n_parts], refs[n_parts:]
    w_ref, tw_ref, table_ref, out_ref, v_buf, hist_buf, sections, z, wide, slabs, sems, out_sems = refs
    keep = mask_ref[0].astype(F32)
    groups = v_buf.shape[0] // 16

    def copies(g, side):
        rows = pl.ds(pl.multiple_of(g * 16, 16), 16)
        jobs = [pltpu.make_async_copy(v_hbm.at[rows], v_buf.at[rows], sems.at[0, g])]
        for k, slot in enumerate(slots):
            part, skip = slot[side]
            source = parts[part].at[pl.ds(pl.multiple_of((g + skip) * 16, 16), 16)]
            jobs.append(pltpu.make_async_copy(source, hist_buf.at[k, rows], sems.at[k + 1, g]))
        return jobs

    for g in range(groups):
        for job in copies(g, g // (groups // 2)):
            job.start()

    def run(taps, side):
        def body(g, carry):
            for job in copies(g, side):
                job.wait()
            rows = pl.ds(pl.multiple_of(g * 16, 16), 16)

            def frames_of(n1, w):
                lanes = slice(n1 * N2, (n1 + 1) * N2)
                v = [v_buf[rows, i * NFFT + n1 * N2 : i * NFFT + (n1 + 1) * N2].astype(F32) for i in range(3)]
                h = [hist_buf[k, rows, lanes].astype(F32) for k in range(len(slots))]
                return taps(keep, w, v, h)

            sections_of(frames_of, n_out, w_ref, sections)
            for f in range(n_out):
                first_half_bins(sections, tw_ref, z, f, f * N2 + g * 16)
            return carry

        return body

    lax.fori_loop(0, groups // 2, run(taps_a, 0), 0)
    lax.fori_loop(groups // 2, groups, run(taps_b, 1), 0)
    emit_slabs(n_out, table_ref, z, wide, slabs, out_ref, out_sems)


def first_a(keep, w, v, h):
    return (w[0] * h[0] + w[1] * v[0] + w[2] * v[1] + w[3] * v[2],)


def first_b(keep, w, v, h):
    return (keep * (w[0] * v[0] + w[1] * v[1] + w[2] * v[2]) + w[3] * h[0],)


def second_a(keep, w, v, h):
    near, one_off, two_off = h
    return (
        keep * (w[0] * v[0] + w[1] * v[1] + w[2] * v[2]) + w[3] * one_off,
        w[0] * two_off + w[1] * near + w[2] * v[0] + w[3] * v[1],
    )


def second_b(keep, w, v, h):
    near, one_off, two_off = h
    return (
        w[0] * one_off + w[1] * v[0] + w[2] * v[1] + w[3] * v[2],
        keep * (w[0] * v[1] + w[1] * v[2]) + w[2] * near + w[3] * two_off,
    )


def spectra_call(n_out, taps_a, taps_b, mask, voltages, parts, slots, window):
    signals = voltages.shape[0]
    n_hist = len(slots)
    rows = CH * 2 * n_out
    vmem = pl.BlockSpec(memory_space=pltpu.VMEM)
    hbm = pl.BlockSpec(memory_space=pltpu.HBM)
    return pl.pallas_call(
        lambda *refs: fft_kernel(n_out, len(parts), slots, taps_a, taps_b, *refs),
        out_shape=jax.ShapeDtypeStruct((rows, N2), BF),
        in_specs=[pl.BlockSpec(memory_space=pltpu.SMEM), hbm] + [hbm] * len(parts) + [vmem] * 3,
        out_specs=hbm,
        scratch_shapes=[
            pltpu.VMEM(voltages.shape, BF),
            pltpu.VMEM((n_hist, signals, NFFT), BF),
            pltpu.VMEM((n_out, 8, 8, 16, N2), F32),
            pltpu.VMEM((NK, 2 * n_out * N2, 2 * N2), BF),
            pltpu.VMEM((rows + NJ, N2), F32),
            pltpu.VMEM((rows, N2), BF),
            pltpu.SemaphoreType.DMA((n_hist + 1, signals // 16)),
            pltpu.SemaphoreType.DMA((NJ,)),
        ],
        cost_estimate=pl.CostEstimate(flops=n_out * 10**10, transcendentals=0, bytes_accessed=n_out * 10**7),
        compiler_params=pltpu.CompilerParams(vmem_limit_bytes=58 * 1024 * 1024),
    )(mask, voltages, *parts, window, jnp.asarray(twiddle_table()), jnp.asarray(bin_table()))


LAP = 2 * N2 + 1


def spread_kernel(in_ref, out_ref, wide):
    def body(t, carry):
        for src in range(2):
            tile = in_ref[pl.ds(pl.multiple_of((t * 2 + src) * 16, 16), 16), :].astype(F32)
            for part in range(2):
                wide[src, pl.ds(part * N2 + t, 8, stride=LAP), :] = tile[part * 8 : part * 8 + 8]
        return carry

    lax.fori_loop(0, N2, body, 0)
    for ch in range(8):
        for src in range(2):
            out_ref[ch, :, src * N2 : (src + 1) * N2] = wide[src, ch * LAP : ch * LAP + 2 * N2, :].astype(BF)


def spread(first):
    vmem = pl.BlockSpec(memory_space=pltpu.VMEM)
    return pl.pallas_call(
        spread_kernel,
        out_shape=jax.ShapeDtypeStruct((8, 2 * N2, 2 * N2), BF),
        in_specs=[vmem],
        out_specs=vmem,
        scratch_shapes=[pltpu.VMEM((2, 8 * LAP + 8, N2), F32)],
        cost_estimate=pl.CostEstimate(flops=2 * 10**9, transcendentals=0, bytes_accessed=10**6),
        compiler_params=pltpu.CompilerParams(vmem_limit_bytes=16 * 1024 * 1024),
    )(first)


def correlate_kernel(own_ref, first_ref, second_ref, out_hbm, send_ref, wide, real, imag, rows_buf, sems):
    own = own_ref[0]
    scale = 1.0 / math.sqrt(3 * N2)
    first_lanes = lax.broadcasted_iota(jnp.int32, (16, N2), 1) < N2 // 2

    def body(t, carry):
        for src in range(2):
            for f in range(2):
                row = pl.multiple_of((t * 2 + src) * 32 + f * 16, 16)
                tile = second_ref[pl.ds(row, 16), :].astype(F32)
                if f:
                    row = pl.multiple_of(((t + N2 - 1) % N2 * 2 + src) * 32 + 16, 16)
                    tile = jnp.where(first_lanes, tile, second_ref[pl.ds(row, 16), :].astype(F32))
                for part in range(2):
                    wide[f, src, pl.ds(part * N2 + t, 8, stride=LAP), :] = tile[part * 8 : part * 8 + 8]
        return carry

    lax.fori_loop(0, N2, body, 0)

    first = own == 0
    mine = pl.ds(pl.multiple_of(own * N2, N2), N2)
    theirs = pl.ds(pl.multiple_of((1 - own) * N2, N2), N2)
    upper = lax.broadcasted_iota(jnp.int32, (N2, N2), 0) <= lax.broadcasted_iota(jnp.int32, (N2, N2), 1)
    half_lanes = lax.broadcasted_iota(jnp.int32, (2 * N2, 2 * N2), 1) % N2 < N2 // 2
    dims = (((0,), (0,)), ((), ()))

    def copy_out(ch):
        return pltpu.make_async_copy(rows_buf.at[ch], out_hbm.at[own * 8 + ch], sems.at[ch])

    for ch in range(8):
        rows = slice(ch * LAP, ch * LAP + 2 * N2)
        g1, g2 = (
            jnp.concatenate([wide[f, 0, rows, :].astype(BF), wide[f, 1, rows, :].astype(BF)], axis=1)
            for f in range(2)
        )
        g0 = first_ref[ch]
        x = [jnp.where(half_lanes, g0, g1), jnp.where(half_lanes, g1, g0), g2]
        xr = jnp.concatenate([part[:N2] for part in x], axis=0)
        xi = jnp.concatenate([part[N2:] for part in x], axis=0)
        both = jnp.concatenate([xr, xi], axis=0)
        p = lax.dot_general(xi, xr, dims, preferred_element_type=F32) * scale
        real[...] = lax.dot_general(both, both, dims, preferred_element_type=F32) * scale
        imag[...] = p - p.T
        rows_buf[ch, :, : 2 * N2] = real[mine, :]
        rows_buf[ch, :, 2 * N2 :] = imag[mine, :]
        copy_out(ch).start()
        rows_r, rows_i = real[theirs, :], imag[theirs, :]
        cross_r = jnp.where(first, rows_r[:, :N2], rows_r[:, N2:])
        cross_i = jnp.where(first, rows_i[:, :N2], rows_i[:, N2:])
        diag_r = jnp.where(first, rows_r[:, N2:], rows_r[:, :N2])
        diag_i = jnp.where(first, rows_i[:, N2:], rows_i[:, :N2])
        send_ref[ch, :, :N2] = cross_r.astype(BF)
        send_ref[ch, :, N2 : 2 * N2] = cross_i.astype(BF)
        send_ref[ch, :, 2 * N2 :] = jnp.where(upper, diag_r, diag_i).astype(BF)

    for ch in range(8):
        copy_out(ch).wait()


def correlate(own, first, second):
    vmem = pl.BlockSpec(memory_space=pltpu.VMEM)
    return pl.pallas_call(
        correlate_kernel,
        out_shape=[
            jax.ShapeDtypeStruct((16, N2, 4 * N2), F32),
            jax.ShapeDtypeStruct((8, N2, 3 * N2), BF),
        ],
        in_specs=[pl.BlockSpec(memory_space=pltpu.SMEM), vmem, vmem],
        out_specs=[pl.BlockSpec(memory_space=pltpu.HBM), vmem],
        scratch_shapes=[
            pltpu.VMEM((2, 2, 8 * LAP + 8, N2), F32),
            pltpu.VMEM((2 * N2, 2 * N2), F32),
            pltpu.VMEM((2 * N2, 2 * N2), F32),
            pltpu.VMEM((8, N2, 4 * N2), F32),
            pltpu.SemaphoreType.DMA((8,)),
        ],
        cost_estimate=pl.CostEstimate(flops=5 * 10**9, transcendentals=0, bytes_accessed=10**7),
        compiler_params=pltpu.CompilerParams(vmem_limit_bytes=40 * 1024 * 1024),
    )(own, first, second)


def finish_kernel(own_ref, part_ref, got_ref, out_hbm, rows_buf, sems):
    own = own_ref[0]
    first = own == 0
    row = lax.broadcasted_iota(jnp.int32, (N2, N2), 0)
    col = lax.broadcasted_iota(jnp.int32, (N2, N2), 1)

    def copy_out(ch):
        return pltpu.make_async_copy(rows_buf.at[ch], out_hbm.at[(1 - own) * 8 + ch], sems.at[ch])

    for ch in range(8):
        cross_r = got_ref[ch, :, :N2].astype(F32)
        cross_i = got_ref[ch, :, N2 : 2 * N2].astype(F32)
        packed = got_ref[ch, :, 2 * N2 :].astype(F32)
        flipped = packed.T
        diag_r = jnp.where(row <= col, packed, flipped)
        diag_i = jnp.where(row > col, packed, jnp.where(row < col, -flipped, 0.0))
        rows_buf[ch, :, :N2] = jnp.where(first, diag_r, cross_r)
        rows_buf[ch, :, N2 : 2 * N2] = jnp.where(first, cross_r, diag_r)
        rows_buf[ch, :, 2 * N2 : 3 * N2] = jnp.where(first, diag_i, cross_i)
        rows_buf[ch, :, 3 * N2 :] = jnp.where(first, cross_i, diag_i)
        copy_out(ch).start()
    for ch in range(8):
        copy_out(ch).wait()


def finish(own, part, got):
    return pl.pallas_call(
        finish_kernel,
        out_shape=jax.ShapeDtypeStruct(part.shape, F32),
        in_specs=[
            pl.BlockSpec(memory_space=pltpu.SMEM),
            pl.BlockSpec(memory_space=pltpu.HBM),
            pl.BlockSpec(memory_space=pltpu.VMEM),
        ],
        out_specs=pl.BlockSpec(memory_space=pltpu.HBM),
        scratch_shapes=[pltpu.VMEM((8, N2, 4 * N2), F32), pltpu.SemaphoreType.DMA((8,))],
        input_output_aliases={1: 0},
        compiler_params=pltpu.CompilerParams(vmem_limit_bytes=8 * 1024 * 1024),
    )(own, part, got)


def cut_kernel(plan, v_hbm, *refs):
    outs, sems = refs[: len(plan)], refs[len(plan)]
    jobs = []
    for out, pieces in zip(outs, plan):
        at = 0
        for (start, stop), frame in pieces:
            for row in range(start, stop, 16):
                source = v_hbm.at[pl.ds(row, 16), pl.ds(frame * NFFT, NFFT)]
                jobs.append(pltpu.make_async_copy(source, out.at[pl.ds(at, 16)], sems.at[len(jobs)]))
                at += 16
    for job in jobs:
        job.start()
    for job in jobs:
        job.wait()


def cut(voltages, plan):
    sizes = [sum(stop - start for (start, stop), _ in pieces) for pieces in plan]
    hbm = pl.BlockSpec(memory_space=pltpu.HBM)
    return pl.pallas_call(
        lambda *refs: cut_kernel(plan, *refs),
        out_shape=[jax.ShapeDtypeStruct((size, NFFT), BF) for size in sizes],
        in_specs=[hbm],
        out_specs=[pl.BlockSpec(memory_space=pltpu.VMEM)] * len(plan),
        scratch_shapes=[pltpu.SemaphoreType.DMA((sum(sizes) // 16,))],
        cost_estimate=pl.CostEstimate(flops=10**9, transcendentals=0, bytes_accessed=10**7),
        compiler_params=pltpu.CompilerParams(vmem_limit_bytes=60 * 1024 * 1024),
    )(voltages)


def per_device(voltages, pfb_window):
    signals = voltages.shape[0]
    peers = lax.axis_size("ta")
    half = signals // 2
    to_right = [(i, i + 1) for i in range(peers - 1)]
    to_left = [(i, (i - 1) % peers) for i in range(peers)]
    inner = (lax.axis_index("ta") < peers - 1).astype(jnp.int32).reshape(1)
    own = lax.axis_index("aa").astype(jnp.int32).reshape(1)
    to_r, to_l = cut(voltages, ((((0, half), 2),), (((half, signals), 0),)))
    prev_a = lax.ppermute(to_r, "ta", to_right)
    next_b = lax.ppermute(to_l, "ta", to_left)
    top, bottom = (0, half), (half, signals)
    to_r, to_l = cut(voltages, (((top, 1), (bottom, 2)), ((top, 0), (bottom, 1))))
    right = lax.ppermute(to_r, "ta", to_right)
    left = lax.ppermute(to_l, "ta", to_left)
    low = -(half // 16)
    near = ((0, 0), (1, low))
    first = spectra_call(1, first_a, first_b, inner, voltages, (prev_a, next_b), (near,), pfb_window)
    first = lax.all_to_all(first, ("ta", "aa"), split_axis=0, concat_axis=0, tiled=True)
    slots = (near, ((2, 0), (3, 0)), ((3, 0), (2, 0)))
    parts = (prev_a, next_b, left, right)
    second = spectra_call(2, second_a, second_b, inner, voltages, parts, slots, pfb_window)
    second = lax.all_to_all(second, ("ta", "aa"), split_axis=0, concat_axis=0, tiled=True)
    first = spread(first)
    part, send = correlate(own, first, second)
    got = lax.ppermute(send, "aa", [(0, 1), (1, 0)])
    return finish(own, part, got)


def solution(mesh):
    return jax.shard_map(
        per_device,
        mesh=mesh,
        in_specs=(P("aa", "ta"), P()),
        out_specs=P("ta", "aa", None),
        check_vma=False,
    )
```

```python
import math

import jax
import jax.numpy as jnp
import numpy as np
from jax import lax
from jax.experimental import pallas as pl
from jax.experimental.pallas import tpu as pltpu
from jax.sharding import PartitionSpec as P

NFFT = 8192
CH = 2048
TAPS = 4
CH_OFF = 1024
N1 = 64
N2 = 128
NK = 33
NJ = CH // N1
K2 = CH_OFF // N1
HALF = math.sqrt(0.5)
UNROLL = 32
BF = jnp.bfloat16
F32 = jnp.float32


def twiddle_table():
    phase = np.outer(np.arange(NK), np.arange(N2)) * (2.0 * np.pi / NFFT)
    return np.stack([np.cos(phase), np.sin(phase)], axis=1).astype(np.float32)


def bin_table():
    scale = 1.0 / math.sqrt(NFFT)
    bins = np.arange(K2, K2 + NJ)
    rows = []
    for bin_set, sign in ((bins, 1.0), (-(bins + 1), -1.0)):
        phase = np.outer(bin_set, np.arange(N2)) % N2 * (2.0 * np.pi / N2)
        cosine, sine = np.cos(phase) * scale, np.sin(phase) * scale
        rows.append(np.concatenate([cosine, sine], axis=1))
        rows.append(sign * np.concatenate([-sine, cosine], axis=1))
    table = np.concatenate(rows, axis=0)
    high = table.astype(BF)
    low = (table - high.astype(np.float64)).astype(BF)
    return np.concatenate([high, low], axis=0).T


def real_dft8(x):
    s0, d0 = x[0] + x[4], x[0] - x[4]
    s1, d1 = x[1] + x[5], x[1] - x[5]
    s2, d2 = x[2] + x[6], x[2] - x[6]
    s3, d3 = x[3] + x[7], x[3] - x[7]
    e0, e1 = s0 + s2, s1 + s3
    u, v = HALF * (d1 - d3), HALF * (d1 + d3)
    return [(e0 + e1, None), (d0 + u, -(d2 + v)), (s0 - s2, s3 - s1), (d0 - u, d2 - v), (e0 - e1, None)]


def complex_dft8(z, first_half=False):
    sr = [z[j][0] + z[j + 4][0] for j in range(4)]
    si = [z[j][1] + z[j + 4][1] for j in range(4)]
    dr = [z[j][0] - z[j + 4][0] for j in range(4)]
    di = [z[j][1] - z[j + 4][1] for j in range(4)]
    out = [None] * 8
    pr, pi = dr[1], di[1]
    dr[1], di[1] = HALF * (pr + pi), HALF * (pi - pr)
    dr[2], di[2] = di[2], -dr[2]
    pr, pi = dr[3], di[3]
    dr[3], di[3] = HALF * (pi - pr), -HALF * (pr + pi)
    for base, (ar, ai) in ((0, (sr, si)), (1, (dr, di))):
        er, ei = ar[0] + ar[2], ai[0] + ai[2]
        fr, fi = ar[1] + ar[3], ai[1] + ai[3]
        gr, gi = ar[0] - ar[2], ai[0] - ai[2]
        hr, hi = ar[1] - ar[3], ai[1] - ai[3]
        out[base] = (er + fr, ei + fi)
        out[base + 2] = (gr + hi, gi - hr)
        if not first_half:
            out[base + 4] = (er - fr, ei - fi)
            out[base + 6] = (gr - hi, gi + hr)
    return out


def first_half_bins(sections, tw_ref, z_ref, frame, row):
    low_row = row + z_ref.shape[1] // 2

    def keep(k1, re, im, conj):
        c, s = tw_ref[k1, 0:1, :], tw_ref[k1, 1:2, :]
        if im is None:
            zr, zi = re * c, -(re * s)
        elif conj:
            zr, zi = re * c - im * s, -(im * c + re * s)
        else:
            zr, zi = re * c + im * s, im * c - re * s
        for part, z in ((0, zr), (1, zi)):
            high = z.astype(BF)
            low = (z - high.astype(F32)).astype(BF)
            lanes = slice(part * N2, (part + 1) * N2)
            z_ref[k1, pl.ds(pl.multiple_of(row, 16), 16), lanes] = high
            z_ref[k1, pl.ds(pl.multiple_of(low_row, 16), 16), lanes] = low

    spectrum = real_dft8([sections[frame, 0, b] for b in range(8)])
    for r in range(5):
        keep(8 * r, spectrum[r][0], spectrum[r][1], False)
    for q in (1, 2, 3):
        z = []
        for b in range(8):
            re, im = sections[frame, 2 * q - 1, b], sections[frame, 2 * q, b]
            if b:
                c, s = math.cos(2 * math.pi * b * q / N1), math.sin(2 * math.pi * b * q / N1)
                re, im = re * c + im * s, im * c - re * s
            z.append((re, im))
        for r, (re, im) in enumerate(complex_dft8(z)):
            k1 = q + 8 * r
            if k1 <= 32:
                keep(k1, re, im, False)
            else:
                keep(N1 - k1, re, im, True)
    z = []
    for b in range(8):
        x = sections[frame, 7, b]
        c, s = math.cos(2 * math.pi * b * 4 / N1), math.sin(2 * math.pi * b * 4 / N1)
        z.append((x * c, x * -s) if b else (x, jnp.zeros_like(x)))
    out = complex_dft8(z, first_half=True)
    for r in range(4):
        keep(4 + 8 * r, out[r][0], out[r][1], False)


def sections_of(frames_of, n_out, w_ref, sections):
    for b in range(8):
        filtered = [[] for _ in range(n_out)]
        for a in range(8):
            n1 = 8 * a + b
            w = [w_ref[k : k + 1, n1 * N2 : (n1 + 1) * N2] for k in range(TAPS)]
            for f, value in enumerate(frames_of(n1, w)):
                filtered[f].append(value)
        for f in range(n_out):
            spectrum = real_dft8(filtered[f])
            sections[f, 0, b] = spectrum[0][0]
            for q in (1, 2, 3):
                sections[f, 2 * q - 1, b] = spectrum[q][0]
                sections[f, 2 * q, b] = spectrum[q][1]
            sections[f, 7, b] = spectrum[4][0]


def emit_slabs(n_out, table_ref, z_ref, wide_ref, slabs_ref, out_ref, out_sems):
    slab = n_out * 16
    block = 8 * slab
    lap = block + 1
    rows = n_out * N2

    def some(first, count, mirror):
        left = z_ref[pl.ds(first, count)].reshape(count * 2 * rows, 2 * N2)
        product = jnp.dot(left, table_ref[...], preferred_element_type=F32)
        for u in range(count):
            k1 = first + u
            high, low = (product[(2 * u + i) * rows : (2 * u + i + 1) * rows] for i in range(2))
            spectrum = high[:, :N2] + high[:, N2:] + low[:, :N2]
            for f in range(n_out):
                flipped = spectrum[f * N2 : (f + 1) * N2].T
                for side in range(2 if mirror else 1):
                    ch = N1 - k1 if side else k1
                    start = (ch >> 3) * slab + (ch & 7) + f * 16
                    for part in range(2):
                        at = (side * 2 + part) * NJ
                        wide_ref[pl.ds(start + part * 8, NJ, stride=lap), :] = flipped[at : at + NJ]

    some(0, 1, False)
    lax.fori_loop(0, (NK - 1) // UNROLL, lambda i, c: (some(1 + i * UNROLL, UNROLL, True), c)[1], 0)

    def copy_out(j):
        rows = pl.ds(pl.multiple_of(j * block, block), block)
        return pltpu.make_async_copy(slabs_ref.at[rows], out_ref.at[rows], out_sems.at[j])

    def narrow(j, carry):
        slabs_ref[pl.ds(pl.multiple_of(j * block, block), block), :] = wide_ref[pl.ds(j * lap, block), :].astype(BF)
        copy_out(j).start()
        return carry

    lax.fori_loop(0, NJ, narrow, 0)

    def drain(j, carry):
        copy_out(j).wait()
        return carry

    lax.fori_loop(0, NJ, drain, 0)


def fft_kernel(n_out, n_parts, slots, taps_a, taps_b, mask_ref, v_hbm, *refs):
    parts, refs = refs[:n_parts], refs[n_parts:]
    w_ref, tw_ref, table_ref, out_ref, v_buf, hist_buf, sections, z, wide, slabs, sems, out_sems = refs
    keep = mask_ref[0].astype(F32)
    groups = v_buf.shape[0] // 16

    def copies(g, side):
        rows = pl.ds(pl.multiple_of(g * 16, 16), 16)
        jobs = [pltpu.make_async_copy(v_hbm.at[rows], v_buf.at[rows], sems.at[0, g])]
        for k, slot in enumerate(slots):
            part, skip = slot[side]
            source = parts[part].at[pl.ds(pl.multiple_of((g + skip) * 16, 16), 16)]
            jobs.append(pltpu.make_async_copy(source, hist_buf.at[k, rows], sems.at[k + 1, g]))
        return jobs

    for g in range(groups):
        for job in copies(g, g // (groups // 2)):
            job.start()

    def run(taps, side):
        def body(g, carry):
            for job in copies(g, side):
                job.wait()
            rows = pl.ds(pl.multiple_of(g * 16, 16), 16)

            def frames_of(n1, w):
                lanes = slice(n1 * N2, (n1 + 1) * N2)
                v = [v_buf[rows, i * NFFT + n1 * N2 : i * NFFT + (n1 + 1) * N2].astype(F32) for i in range(3)]
                h = [hist_buf[k, rows, lanes].astype(F32) for k in range(len(slots))]
                return taps(keep, w, v, h)

            sections_of(frames_of, n_out, w_ref, sections)
            for f in range(n_out):
                first_half_bins(sections, tw_ref, z, f, f * N2 + g * 16)
            return carry

        return body

    lax.fori_loop(0, groups // 2, run(taps_a, 0), 0)
    lax.fori_loop(groups // 2, groups, run(taps_b, 1), 0)
    emit_slabs(n_out, table_ref, z, wide, slabs, out_ref, out_sems)


def first_a(keep, w, v, h):
    return (w[0] * h[0] + w[1] * v[0] + w[2] * v[1] + w[3] * v[2],)


def first_b(keep, w, v, h):
    return (keep * (w[0] * v[0] + w[1] * v[1] + w[2] * v[2]) + w[3] * h[0],)


def second_a(keep, w, v, h):
    near, one_off, two_off = h
    return (
        keep * (w[0] * v[0] + w[1] * v[1] + w[2] * v[2]) + w[3] * one_off,
        w[0] * two_off + w[1] * near + w[2] * v[0] + w[3] * v[1],
    )


def second_b(keep, w, v, h):
    near, one_off, two_off = h
    return (
        w[0] * one_off + w[1] * v[0] + w[2] * v[1] + w[3] * v[2],
        keep * (w[0] * v[1] + w[1] * v[2]) + w[2] * near + w[3] * two_off,
    )


def spectra_call(n_out, taps_a, taps_b, mask, voltages, parts, slots, window):
    signals = voltages.shape[0]
    n_hist = len(slots)
    rows = CH * 2 * n_out
    vmem = pl.BlockSpec(memory_space=pltpu.VMEM)
    hbm = pl.BlockSpec(memory_space=pltpu.HBM)
    return pl.pallas_call(
        lambda *refs: fft_kernel(n_out, len(parts), slots, taps_a, taps_b, *refs),
        out_shape=jax.ShapeDtypeStruct((rows, N2), BF),
        in_specs=[pl.BlockSpec(memory_space=pltpu.SMEM), hbm] + [hbm] * len(parts) + [vmem] * 3,
        out_specs=hbm,
        scratch_shapes=[
            pltpu.VMEM(voltages.shape, BF),
            pltpu.VMEM((n_hist, signals, NFFT), BF),
            pltpu.VMEM((n_out, 8, 8, 16, N2), F32),
            pltpu.VMEM((NK, 2 * n_out * N2, 2 * N2), BF),
            pltpu.VMEM((rows + NJ, N2), F32),
            pltpu.VMEM((rows, N2), BF),
            pltpu.SemaphoreType.DMA((n_hist + 1, signals // 16)),
            pltpu.SemaphoreType.DMA((NJ,)),
        ],
        cost_estimate=pl.CostEstimate(flops=n_out * 10**10, transcendentals=0, bytes_accessed=n_out * 10**7),
        compiler_params=pltpu.CompilerParams(vmem_limit_bytes=127 * 512 * 1024),
    )(mask, voltages, *parts, window, jnp.asarray(twiddle_table()), jnp.asarray(bin_table()))


LAP = 2 * N2 + 1


def spread_kernel(in_ref, out_ref, wide):
    def body(t, carry):
        for src in range(2):
            tile = in_ref[pl.ds(pl.multiple_of((t * 2 + src) * 16, 16), 16), :].astype(F32)
            for part in range(2):
                wide[src, pl.ds(part * N2 + t, 8, stride=LAP), :] = tile[part * 8 : part * 8 + 8]
        return carry

    lax.fori_loop(0, N2, body, 0, unroll=4)
    for ch in range(8):
        for src in range(2):
            out_ref[ch, :, src * N2 : (src + 1) * N2] = wide[src, ch * LAP : ch * LAP + 2 * N2, :].astype(BF)


def spread(first):
    vmem = pl.BlockSpec(memory_space=pltpu.VMEM)
    return pl.pallas_call(
        spread_kernel,
        out_shape=jax.ShapeDtypeStruct((8, 2 * N2, 2 * N2), BF),
        in_specs=[vmem],
        out_specs=vmem,
        scratch_shapes=[pltpu.VMEM((2, 8 * LAP + 8, N2), F32)],
        cost_estimate=pl.CostEstimate(flops=2 * 10**9, transcendentals=0, bytes_accessed=10**6),
        compiler_params=pltpu.CompilerParams(vmem_limit_bytes=16 * 1024 * 1024),
    )(first)


def correlate_kernel(own_ref, first_ref, second_ref, out_hbm, send_ref, wide, real, imag, rows_buf, sems):
    own = own_ref[0]
    scale = 1.0 / math.sqrt(3 * N2)
    first_lanes = lax.broadcasted_iota(jnp.int32, (16, N2), 1) < N2 // 2

    def body(t, carry):
        for src in range(2):
            for f in range(2):
                row = pl.multiple_of((t * 2 + src) * 32 + f * 16, 16)
                tile = second_ref[pl.ds(row, 16), :].astype(F32)
                if f:
                    row = pl.multiple_of(((t + N2 - 1) % N2 * 2 + src) * 32 + 16, 16)
                    tile = jnp.where(first_lanes, tile, second_ref[pl.ds(row, 16), :].astype(F32))
                for part in range(2):
                    wide[f, src, pl.ds(part * N2 + t, 8, stride=LAP), :] = tile[part * 8 : part * 8 + 8]
        return carry

    lax.fori_loop(0, N2, body, 0, unroll=4)

    first = own == 0
    mine = pl.ds(pl.multiple_of(own * N2, N2), N2)
    theirs = pl.ds(pl.multiple_of((1 - own) * N2, N2), N2)
    upper = lax.broadcasted_iota(jnp.int32, (N2, N2), 0) <= lax.broadcasted_iota(jnp.int32, (N2, N2), 1)
    half_lanes = lax.broadcasted_iota(jnp.int32, (2 * N2, 2 * N2), 1) % N2 < N2 // 2
    dims = (((0,), (0,)), ((), ()))

    def copy_out(ch):
        return pltpu.make_async_copy(rows_buf.at[ch], out_hbm.at[own * 8 + ch], sems.at[ch])

    for ch in range(8):
        rows = slice(ch * LAP, ch * LAP + 2 * N2)
        g1, g2 = (
            jnp.concatenate([wide[f, 0, rows, :].astype(BF), wide[f, 1, rows, :].astype(BF)], axis=1)
            for f in range(2)
        )
        g0 = first_ref[ch]
        x = [jnp.where(half_lanes, g0, g1), jnp.where(half_lanes, g1, g0), g2]
        xr = jnp.concatenate([part[:N2] for part in x], axis=0)
        xi = jnp.concatenate([part[N2:] for part in x], axis=0)
        both = jnp.concatenate([xr, xi], axis=0)
        p = lax.dot_general(xi, xr, dims, preferred_element_type=F32) * scale
        real[...] = lax.dot_general(both, both, dims, preferred_element_type=F32) * scale
        imag[...] = p - p.T
        rows_buf[ch, :, : 2 * N2] = real[mine, :]
        rows_buf[ch, :, 2 * N2 :] = imag[mine, :]
        copy_out(ch).start()
        rows_r, rows_i = real[theirs, :], imag[theirs, :]
        cross_r = jnp.where(first, rows_r[:, :N2], rows_r[:, N2:])
        cross_i = jnp.where(first, rows_i[:, :N2], rows_i[:, N2:])
        diag_r = jnp.where(first, rows_r[:, N2:], rows_r[:, :N2])
        diag_i = jnp.where(first, rows_i[:, N2:], rows_i[:, :N2])
        send_ref[ch, :, :N2] = cross_r.astype(BF)
        send_ref[ch, :, N2 : 2 * N2] = cross_i.astype(BF)
        send_ref[ch, :, 2 * N2 :] = jnp.where(upper, diag_r, diag_i).astype(BF)

    for ch in range(8):
        copy_out(ch).wait()


def correlate(own, first, second):
    vmem = pl.BlockSpec(memory_space=pltpu.VMEM)
    return pl.pallas_call(
        correlate_kernel,
        out_shape=[
            jax.ShapeDtypeStruct((16, N2, 4 * N2), F32),
            jax.ShapeDtypeStruct((8, N2, 3 * N2), BF),
        ],
        in_specs=[pl.BlockSpec(memory_space=pltpu.SMEM), vmem, vmem],
        out_specs=[pl.BlockSpec(memory_space=pltpu.HBM), vmem],
        scratch_shapes=[
            pltpu.VMEM((2, 2, 8 * LAP + 8, N2), F32),
            pltpu.VMEM((2 * N2, 2 * N2), F32),
            pltpu.VMEM((2 * N2, 2 * N2), F32),
            pltpu.VMEM((8, N2, 4 * N2), F32),
            pltpu.SemaphoreType.DMA((8,)),
        ],
        cost_estimate=pl.CostEstimate(flops=5 * 10**9, transcendentals=0, bytes_accessed=10**7),
        compiler_params=pltpu.CompilerParams(vmem_limit_bytes=40 * 1024 * 1024),
    )(own, first, second)


def finish_kernel(own_ref, part_ref, got_ref, out_hbm, rows_buf, sems):
    own = own_ref[0]
    first = own == 0
    row = lax.broadcasted_iota(jnp.int32, (N2, N2), 0)
    col = lax.broadcasted_iota(jnp.int32, (N2, N2), 1)

    def copy_out(ch):
        return pltpu.make_async_copy(rows_buf.at[ch], out_hbm.at[(1 - own) * 8 + ch], sems.at[ch])

    for ch in range(8):
        cross_r = got_ref[ch, :, :N2].astype(F32)
        cross_i = got_ref[ch, :, N2 : 2 * N2].astype(F32)
        packed = got_ref[ch, :, 2 * N2 :].astype(F32)
        flipped = packed.T
        diag_r = jnp.where(row <= col, packed, flipped)
        diag_i = jnp.where(row > col, packed, jnp.where(row < col, -flipped, 0.0))
        rows_buf[ch, :, :N2] = jnp.where(first, diag_r, cross_r)
        rows_buf[ch, :, N2 : 2 * N2] = jnp.where(first, cross_r, diag_r)
        rows_buf[ch, :, 2 * N2 : 3 * N2] = jnp.where(first, diag_i, cross_i)
        rows_buf[ch, :, 3 * N2 :] = jnp.where(first, cross_i, diag_i)
        copy_out(ch).start()
    for ch in range(8):
        copy_out(ch).wait()


def finish(own, part, got):
    return pl.pallas_call(
        finish_kernel,
        out_shape=jax.ShapeDtypeStruct(part.shape, F32),
        in_specs=[
            pl.BlockSpec(memory_space=pltpu.SMEM),
            pl.BlockSpec(memory_space=pltpu.HBM),
            pl.BlockSpec(memory_space=pltpu.VMEM),
        ],
        out_specs=pl.BlockSpec(memory_space=pltpu.HBM),
        scratch_shapes=[pltpu.VMEM((8, N2, 4 * N2), F32), pltpu.SemaphoreType.DMA((8,))],
        input_output_aliases={1: 0},
        compiler_params=pltpu.CompilerParams(vmem_limit_bytes=8 * 1024 * 1024),
    )(own, part, got)


def cut_kernel(plan, v_hbm, *refs):
    outs, sems = refs[: len(plan)], refs[len(plan)]
    jobs = []
    for out, pieces in zip(outs, plan):
        at = 0
        for (start, stop), frame in pieces:
            for row in range(start, stop, 16):
                source = v_hbm.at[pl.ds(row, 16), pl.ds(frame * NFFT, NFFT)]
                jobs.append(pltpu.make_async_copy(source, out.at[pl.ds(at, 16)], sems.at[len(jobs)]))
                at += 16
    for job in jobs:
        job.start()
    for job in jobs:
        job.wait()


def cut(voltages, plan):
    sizes = [sum(stop - start for (start, stop), _ in pieces) for pieces in plan]
    hbm = pl.BlockSpec(memory_space=pltpu.HBM)
    return pl.pallas_call(
        lambda *refs: cut_kernel(plan, *refs),
        out_shape=[jax.ShapeDtypeStruct((size, NFFT), BF) for size in sizes],
        in_specs=[hbm],
        out_specs=[pl.BlockSpec(memory_space=pltpu.VMEM)] * len(plan),
        scratch_shapes=[pltpu.SemaphoreType.DMA((sum(sizes) // 16,))],
        cost_estimate=pl.CostEstimate(flops=10**9, transcendentals=0, bytes_accessed=10**7),
        compiler_params=pltpu.CompilerParams(vmem_limit_bytes=127 * 512 * 1024),
    )(voltages)


def per_device(voltages, pfb_window):
    signals = voltages.shape[0]
    peers = lax.axis_size("ta")
    half = signals // 2
    to_right = [(i, i + 1) for i in range(peers - 1)]
    to_left = [(i, (i - 1) % peers) for i in range(peers)]
    inner = (lax.axis_index("ta") < peers - 1).astype(jnp.int32).reshape(1)
    own = lax.axis_index("aa").astype(jnp.int32).reshape(1)
    to_r, to_l = cut(voltages, ((((0, half), 2),), (((half, signals), 0),)))
    prev_a = lax.ppermute(to_r, "ta", to_right)
    next_b = lax.ppermute(to_l, "ta", to_left)
    top, bottom = (0, half), (half, signals)
    to_r, to_l = cut(voltages, (((top, 1), (bottom, 2)), ((top, 0), (bottom, 1))))
    right = lax.ppermute(to_r, "ta", to_right)
    left = lax.ppermute(to_l, "ta", to_left)
    low = -(half // 16)
    near = ((0, 0), (1, low))
    first = spectra_call(1, first_a, first_b, inner, voltages, (prev_a, next_b), (near,), pfb_window)
    first = lax.all_to_all(first, ("ta", "aa"), split_axis=0, concat_axis=0, tiled=True)
    slots = (near, ((2, 0), (3, 0)), ((3, 0), (2, 0)))
    parts = (prev_a, next_b, left, right)
    second = spectra_call(2, second_a, second_b, inner, voltages, parts, slots, pfb_window)
    second = lax.all_to_all(second, ("ta", "aa"), split_axis=0, concat_axis=0, tiled=True)
    first = spread(first)
    part, send = correlate(own, first, second)
    got = lax.ppermute(send, "aa", [(0, 1), (1, 0)])
    return finish(own, part, got)


def solution(mesh):
    return jax.shard_map(
        per_device,
        mesh=mesh,
        in_specs=(P("aa", "ta"), P()),
        out_specs=P("ta", "aa", None),
        check_vma=False,
    )
```

```python
import math

import jax
import jax.numpy as jnp
import numpy as np
from jax import lax
from jax.experimental import pallas as pl
from jax.experimental.pallas import tpu as pltpu
from jax.sharding import PartitionSpec as P

NFFT = 8192
CH = 2048
TAPS = 4
CH_OFF = 1024
N1 = 64
N2 = 128
NK = 33
NJ = CH // N1
K2 = CH_OFF // N1
HALF = math.sqrt(0.5)
UNROLL = 32
BF = jnp.bfloat16
F32 = jnp.float32


def twiddle_table():
    phase = np.outer(np.arange(NK), np.arange(N2)) * (2.0 * np.pi / NFFT)
    return np.stack([np.cos(phase), np.sin(phase)], axis=1).astype(np.float32)


def bin_table():
    scale = 1.0 / math.sqrt(NFFT)
    bins = np.arange(K2, K2 + NJ)
    rows = []
    for bin_set, sign in ((bins, 1.0), (-(bins + 1), -1.0)):
        phase = np.outer(bin_set, np.arange(N2)) % N2 * (2.0 * np.pi / N2)
        cosine, sine = np.cos(phase) * scale, np.sin(phase) * scale
        rows.append(np.concatenate([cosine, sine], axis=1))
        rows.append(sign * np.concatenate([-sine, cosine], axis=1))
    table = np.concatenate(rows, axis=0)
    high = table.astype(BF)
    low = (table - high.astype(np.float64)).astype(BF)
    return np.concatenate([high, low], axis=0).T


def real_dft8(x):
    s0, d0 = x[0] + x[4], x[0] - x[4]
    s1, d1 = x[1] + x[5], x[1] - x[5]
    s2, d2 = x[2] + x[6], x[2] - x[6]
    s3, d3 = x[3] + x[7], x[3] - x[7]
    e0, e1 = s0 + s2, s1 + s3
    u, v = HALF * (d1 - d3), HALF * (d1 + d3)
    return [(e0 + e1, None), (d0 + u, -(d2 + v)), (s0 - s2, s3 - s1), (d0 - u, d2 - v), (e0 - e1, None)]


def complex_dft8(z, first_half=False):
    sr = [z[j][0] + z[j + 4][0] for j in range(4)]
    si = [z[j][1] + z[j + 4][1] for j in range(4)]
    dr = [z[j][0] - z[j + 4][0] for j in range(4)]
    di = [z[j][1] - z[j + 4][1] for j in range(4)]
    out = [None] * 8
    pr, pi = dr[1], di[1]
    dr[1], di[1] = HALF * (pr + pi), HALF * (pi - pr)
    dr[2], di[2] = di[2], -dr[2]
    pr, pi = dr[3], di[3]
    dr[3], di[3] = HALF * (pi - pr), -HALF * (pr + pi)
    for base, (ar, ai) in ((0, (sr, si)), (1, (dr, di))):
        er, ei = ar[0] + ar[2], ai[0] + ai[2]
        fr, fi = ar[1] + ar[3], ai[1] + ai[3]
        gr, gi = ar[0] - ar[2], ai[0] - ai[2]
        hr, hi = ar[1] - ar[3], ai[1] - ai[3]
        out[base] = (er + fr, ei + fi)
        out[base + 2] = (gr + hi, gi - hr)
        if not first_half:
            out[base + 4] = (er - fr, ei - fi)
            out[base + 6] = (gr - hi, gi + hr)
    return out


def first_half_bins(sections, tw_ref, z_ref, frame, row):
    low_row = row + z_ref.shape[1] // 2

    def keep(k1, re, im, conj):
        c, s = tw_ref[k1, 0:1, :], tw_ref[k1, 1:2, :]
        if im is None:
            zr, zi = re * c, -(re * s)
        elif conj:
            zr, zi = re * c - im * s, -(im * c + re * s)
        else:
            zr, zi = re * c + im * s, im * c - re * s
        for part, z in ((0, zr), (1, zi)):
            high = z.astype(BF)
            low = (z - high.astype(F32)).astype(BF)
            lanes = slice(part * N2, (part + 1) * N2)
            z_ref[k1, pl.ds(pl.multiple_of(row, 16), 16), lanes] = high
            z_ref[k1, pl.ds(pl.multiple_of(low_row, 16), 16), lanes] = low

    spectrum = real_dft8([sections[frame, 0, b] for b in range(8)])
    for r in range(5):
        keep(8 * r, spectrum[r][0], spectrum[r][1], False)
    for q in (1, 2, 3):
        z = []
        for b in range(8):
            re, im = sections[frame, 2 * q - 1, b], sections[frame, 2 * q, b]
            if b:
                c, s = math.cos(2 * math.pi * b * q / N1), math.sin(2 * math.pi * b * q / N1)
                re, im = re * c + im * s, im * c - re * s
            z.append((re, im))
        for r, (re, im) in enumerate(complex_dft8(z)):
            k1 = q + 8 * r
            if k1 <= 32:
                keep(k1, re, im, False)
            else:
                keep(N1 - k1, re, im, True)
    z = []
    for b in range(8):
        x = sections[frame, 7, b]
        c, s = math.cos(2 * math.pi * b * 4 / N1), math.sin(2 * math.pi * b * 4 / N1)
        z.append((x * c, x * -s) if b else (x, jnp.zeros_like(x)))
    out = complex_dft8(z, first_half=True)
    for r in range(4):
        keep(4 + 8 * r, out[r][0], out[r][1], False)


def sections_of(frames_of, n_out, w_ref, sections):
    for b in range(8):
        filtered = [[] for _ in range(n_out)]
        for a in range(8):
            n1 = 8 * a + b
            w = [w_ref[k : k + 1, n1 * N2 : (n1 + 1) * N2] for k in range(TAPS)]
            for f, value in enumerate(frames_of(n1, w)):
                filtered[f].append(value)
        for f in range(n_out):
            spectrum = real_dft8(filtered[f])
            sections[f, 0, b] = spectrum[0][0]
            for q in (1, 2, 3):
                sections[f, 2 * q - 1, b] = spectrum[q][0]
                sections[f, 2 * q, b] = spectrum[q][1]
            sections[f, 7, b] = spectrum[4][0]


def emit_slabs(n_out, table_ref, z_ref, wide_ref, slabs_ref, out_ref, out_sems):
    slab = n_out * 16
    block = 8 * slab
    lap = block + 1
    rows = n_out * N2

    def some(first, count, mirror):
        left = z_ref[pl.ds(first, count)].reshape(count * 2 * rows, 2 * N2)
        product = jnp.dot(left, table_ref[...], preferred_element_type=F32)
        for u in range(count):
            k1 = first + u
            high, low = (product[(2 * u + i) * rows : (2 * u + i + 1) * rows] for i in range(2))
            spectrum = high[:, :N2] + high[:, N2:] + low[:, :N2]
            for f in range(n_out):
                flipped = spectrum[f * N2 : (f + 1) * N2].T
                for side in range(2 if mirror else 1):
                    ch = N1 - k1 if side else k1
                    start = (ch >> 3) * slab + (ch & 7) + f * 16
                    for part in range(2):
                        at = (side * 2 + part) * NJ
                        wide_ref[pl.ds(start + part * 8, NJ, stride=lap), :] = flipped[at : at + NJ]

    some(0, 1, False)
    lax.fori_loop(0, (NK - 1) // UNROLL, lambda i, c: (some(1 + i * UNROLL, UNROLL, True), c)[1], 0)

    def copy_out(j):
        rows = pl.ds(pl.multiple_of(j * block, block), block)
        return pltpu.make_async_copy(slabs_ref.at[rows], out_ref.at[rows], out_sems.at[j])

    def narrow(j, carry):
        slabs_ref[pl.ds(pl.multiple_of(j * block, block), block), :] = wide_ref[pl.ds(j * lap, block), :].astype(BF)
        copy_out(j).start()
        return carry

    lax.fori_loop(0, NJ, narrow, 0)

    def drain(j, carry):
        copy_out(j).wait()
        return carry

    lax.fori_loop(0, NJ, drain, 0)


def fft_kernel(n_out, n_parts, slots, taps_a, taps_b, mask_ref, v_hbm, *refs):
    parts, refs = refs[:n_parts], refs[n_parts:]
    w_ref, tw_ref, table_ref, out_ref, v_buf, hist_buf, sections, z, wide, slabs, sems, out_sems = refs
    keep = mask_ref[0].astype(F32)
    groups = v_buf.shape[0] // 16

    def copies(g, side):
        rows = pl.ds(pl.multiple_of(g * 16, 16), 16)
        jobs = [pltpu.make_async_copy(v_hbm.at[rows], v_buf.at[rows], sems.at[0, g])]
        for k, slot in enumerate(slots):
            part, skip = slot[side]
            source = parts[part].at[pl.ds(pl.multiple_of((g + skip) * 16, 16), 16)]
            jobs.append(pltpu.make_async_copy(source, hist_buf.at[k, rows], sems.at[k + 1, g]))
        return jobs

    for g in range(groups):
        for job in copies(g, g // (groups // 2)):
            job.start()

    def run(taps, side):
        def body(g, carry):
            for job in copies(g, side):
                job.wait()
            rows = pl.ds(pl.multiple_of(g * 16, 16), 16)

            def frames_of(n1, w):
                lanes = slice(n1 * N2, (n1 + 1) * N2)
                v = [v_buf[rows, i * NFFT + n1 * N2 : i * NFFT + (n1 + 1) * N2].astype(F32) for i in range(3)]
                h = [hist_buf[k, rows, lanes].astype(F32) for k in range(len(slots))]
                return taps(keep, w, v, h)

            sections_of(frames_of, n_out, w_ref, sections)
            for f in range(n_out):
                first_half_bins(sections, tw_ref, z, f, f * N2 + g * 16)
            return carry

        return body

    lax.fori_loop(0, groups // 2, run(taps_a, 0), 0)
    lax.fori_loop(groups // 2, groups, run(taps_b, 1), 0)
    emit_slabs(n_out, table_ref, z, wide, slabs, out_ref, out_sems)


def first_a(keep, w, v, h):
    return (w[0] * h[0] + w[1] * v[0] + w[2] * v[1] + w[3] * v[2],)


def first_b(keep, w, v, h):
    return (keep * (w[0] * v[0] + w[1] * v[1] + w[2] * v[2]) + w[3] * h[0],)


def second_a(keep, w, v, h):
    near, one_off, two_off = h
    return (
        keep * (w[0] * v[0] + w[1] * v[1] + w[2] * v[2]) + w[3] * one_off,
        w[0] * two_off + w[1] * near + w[2] * v[0] + w[3] * v[1],
    )


def second_b(keep, w, v, h):
    near, one_off, two_off = h
    return (
        w[0] * one_off + w[1] * v[0] + w[2] * v[1] + w[3] * v[2],
        keep * (w[0] * v[1] + w[1] * v[2]) + w[2] * near + w[3] * two_off,
    )


def spectra_call(n_out, taps_a, taps_b, mask, voltages, parts, slots, window):
    signals = voltages.shape[0]
    n_hist = len(slots)
    rows = CH * 2 * n_out
    vmem = pl.BlockSpec(memory_space=pltpu.VMEM)
    hbm = pl.BlockSpec(memory_space=pltpu.HBM)
    return pl.pallas_call(
        lambda *refs: fft_kernel(n_out, len(parts), slots, taps_a, taps_b, *refs),
        out_shape=jax.ShapeDtypeStruct((rows, N2), BF),
        in_specs=[pl.BlockSpec(memory_space=pltpu.SMEM), hbm] + [hbm] * len(parts) + [vmem] * 3,
        out_specs=hbm,
        scratch_shapes=[
            pltpu.VMEM(voltages.shape, BF),
            pltpu.VMEM((n_hist, signals, NFFT), BF),
            pltpu.VMEM((n_out, 8, 8, 16, N2), F32),
            pltpu.VMEM((NK, 2 * n_out * N2, 2 * N2), BF),
            pltpu.VMEM((rows + NJ, N2), F32),
            pltpu.VMEM((rows, N2), BF),
            pltpu.SemaphoreType.DMA((n_hist + 1, signals // 16)),
            pltpu.SemaphoreType.DMA((NJ,)),
        ],
        cost_estimate=pl.CostEstimate(flops=n_out * 10**10, transcendentals=0, bytes_accessed=n_out * 10**7),
        compiler_params=pltpu.CompilerParams(vmem_limit_bytes=127 * 512 * 1024),
    )(mask, voltages, *parts, window, jnp.asarray(twiddle_table()), jnp.asarray(bin_table()))


LAP = 2 * N2 + 1


def spread_kernel(in_ref, out_ref, wide):
    def body(t, carry):
        for src in range(2):
            tile = in_ref[pl.ds(pl.multiple_of((t * 2 + src) * 16, 16), 16), :].astype(F32)
            for part in range(2):
                wide[src, pl.ds(part * N2 + t, 8, stride=LAP), :] = tile[part * 8 : part * 8 + 8]
        return carry

    lax.fori_loop(0, N2, body, 0, unroll=4)
    for ch in range(8):
        for src in range(2):
            out_ref[ch, :, src * N2 : (src + 1) * N2] = wide[src, ch * LAP : ch * LAP + 2 * N2, :].astype(BF)


def spread(first):
    vmem = pl.BlockSpec(memory_space=pltpu.VMEM)
    return pl.pallas_call(
        spread_kernel,
        out_shape=jax.ShapeDtypeStruct((8, 2 * N2, 2 * N2), BF),
        in_specs=[vmem],
        out_specs=vmem,
        scratch_shapes=[pltpu.VMEM((2, 8 * LAP + 8, N2), F32)],
        cost_estimate=pl.CostEstimate(flops=2 * 10**9, transcendentals=0, bytes_accessed=10**6),
        compiler_params=pltpu.CompilerParams(vmem_limit_bytes=16 * 1024 * 1024),
    )(first)


def correlate_kernel(own_ref, first_ref, second_ref, out_hbm, send_ref, wide, real, imag, rows_buf, sems):
    own = own_ref[0]
    scale = 1.0 / math.sqrt(3 * N2)
    first_lanes = lax.broadcasted_iota(jnp.int32, (16, N2), 1) < N2 // 2

    def body(t, carry):
        for src in range(2):
            for f in range(2):
                row = pl.multiple_of((t * 2 + src) * 32 + f * 16, 16)
                tile = second_ref[pl.ds(row, 16), :].astype(F32)
                if f:
                    row = pl.multiple_of(((t + N2 - 1) % N2 * 2 + src) * 32 + 16, 16)
                    tile = jnp.where(first_lanes, tile, second_ref[pl.ds(row, 16), :].astype(F32))
                for part in range(2):
                    wide[f, src, pl.ds(part * N2 + t, 8, stride=LAP), :] = tile[part * 8 : part * 8 + 8]
        return carry

    lax.fori_loop(0, N2, body, 0, unroll=4)

    first = own == 0
    mine = pl.ds(pl.multiple_of(own * N2, N2), N2)
    theirs = pl.ds(pl.multiple_of((1 - own) * N2, N2), N2)
    upper = lax.broadcasted_iota(jnp.int32, (N2, N2), 0) <= lax.broadcasted_iota(jnp.int32, (N2, N2), 1)
    half_lanes = lax.broadcasted_iota(jnp.int32, (2 * N2, 2 * N2), 1) % N2 < N2 // 2
    dims = (((0,), (0,)), ((), ()))

    def copy_out(ch):
        return pltpu.make_async_copy(rows_buf.at[ch], out_hbm.at[own * 8 + ch], sems.at[ch])

    for ch in range(8):
        rows = slice(ch * LAP, ch * LAP + 2 * N2)
        g1, g2 = (
            jnp.concatenate([wide[f, 0, rows, :].astype(BF), wide[f, 1, rows, :].astype(BF)], axis=1)
            for f in range(2)
        )
        g0 = first_ref[ch]
        x = [jnp.where(half_lanes, g0, g1), jnp.where(half_lanes, g1, g0), g2]
        xr = jnp.concatenate([part[:N2] for part in x], axis=0)
        xi = jnp.concatenate([part[N2:] for part in x], axis=0)
        both = jnp.concatenate([xr, xi], axis=0)
        p = lax.dot_general(xi, xr, dims, preferred_element_type=F32) * scale
        real[...] = lax.dot_general(both, both, dims, preferred_element_type=F32) * scale
        imag[...] = p - p.T
        rows_buf[ch, :, : 2 * N2] = real[mine, :]
        rows_buf[ch, :, 2 * N2 :] = imag[mine, :]
        copy_out(ch).start()
        rows_r, rows_i = real[theirs, :], imag[theirs, :]
        cross_r = jnp.where(first, rows_r[:, :N2], rows_r[:, N2:])
        cross_i = jnp.where(first, rows_i[:, :N2], rows_i[:, N2:])
        diag_r = jnp.where(first, rows_r[:, N2:], rows_r[:, :N2])
        diag_i = jnp.where(first, rows_i[:, N2:], rows_i[:, :N2])
        send_ref[ch, :, :N2] = cross_r.astype(BF)
        send_ref[ch, :, N2 : 2 * N2] = cross_i.astype(BF)
        send_ref[ch, :, 2 * N2 :] = jnp.where(upper, diag_r, diag_i).astype(BF)

    for ch in range(8):
        copy_out(ch).wait()


def correlate(own, first, second):
    vmem = pl.BlockSpec(memory_space=pltpu.VMEM)
    return pl.pallas_call(
        correlate_kernel,
        out_shape=[
            jax.ShapeDtypeStruct((16, N2, 4 * N2), F32),
            jax.ShapeDtypeStruct((8, N2, 3 * N2), BF),
        ],
        in_specs=[pl.BlockSpec(memory_space=pltpu.SMEM), vmem, vmem],
        out_specs=[pl.BlockSpec(memory_space=pltpu.HBM), vmem],
        scratch_shapes=[
            pltpu.VMEM((2, 2, 8 * LAP + 8, N2), F32),
            pltpu.VMEM((2 * N2, 2 * N2), F32),
            pltpu.VMEM((2 * N2, 2 * N2), F32),
            pltpu.VMEM((8, N2, 4 * N2), F32),
            pltpu.SemaphoreType.DMA((8,)),
        ],
        cost_estimate=pl.CostEstimate(flops=5 * 10**9, transcendentals=0, bytes_accessed=10**7),
        compiler_params=pltpu.CompilerParams(vmem_limit_bytes=40 * 1024 * 1024),
    )(own, first, second)


def finish_kernel(own_ref, part_ref, got_ref, out_hbm, rows_buf, sems):
    own = own_ref[0]
    first = own == 0
    row = lax.broadcasted_iota(jnp.int32, (N2, N2), 0)
    col = lax.broadcasted_iota(jnp.int32, (N2, N2), 1)

    def copy_out(ch):
        return pltpu.make_async_copy(rows_buf.at[ch], out_hbm.at[(1 - own) * 8 + ch], sems.at[ch])

    for ch in range(8):
        cross_r = got_ref[ch, :, :N2].astype(F32)
        cross_i = got_ref[ch, :, N2 : 2 * N2].astype(F32)
        packed = got_ref[ch, :, 2 * N2 :].astype(F32)
        flipped = packed.T
        diag_r = jnp.where(row <= col, packed, flipped)
        diag_i = jnp.where(row > col, packed, jnp.where(row < col, -flipped, 0.0))
        rows_buf[ch, :, :N2] = jnp.where(first, diag_r, cross_r)
        rows_buf[ch, :, N2 : 2 * N2] = jnp.where(first, cross_r, diag_r)
        rows_buf[ch, :, 2 * N2 : 3 * N2] = jnp.where(first, diag_i, cross_i)
        rows_buf[ch, :, 3 * N2 :] = jnp.where(first, cross_i, diag_i)
        copy_out(ch).start()
    for ch in range(8):
        copy_out(ch).wait()


def finish(own, part, got):
    return pl.pallas_call(
        finish_kernel,
        out_shape=jax.ShapeDtypeStruct(part.shape, F32),
        in_specs=[
            pl.BlockSpec(memory_space=pltpu.SMEM),
            pl.BlockSpec(memory_space=pltpu.HBM),
            pl.BlockSpec(memory_space=pltpu.VMEM),
        ],
        out_specs=pl.BlockSpec(memory_space=pltpu.HBM),
        scratch_shapes=[pltpu.VMEM((8, N2, 4 * N2), F32), pltpu.SemaphoreType.DMA((8,))],
        input_output_aliases={1: 0},
        compiler_params=pltpu.CompilerParams(vmem_limit_bytes=8 * 1024 * 1024),
    )(own, part, got)


def cut_kernel(plan, v_hbm, *refs):
    outs, (buf, in_sems, out_sems) = refs[: len(plan)], refs[len(plan) :]
    jobs = []
    for out, pieces in zip(outs, plan):
        at = 0
        for (start, stop), frame in pieces:
            for row in range(start, stop, 16):
                i = len(jobs)
                source = v_hbm.at[pl.ds(row, 16), pl.ds(frame * NFFT, NFFT)]
                fetch = pltpu.make_async_copy(source, buf.at[i], in_sems.at[i])
                put = pltpu.make_async_copy(buf.at[i], out.at[pl.ds(at, 16)], out_sems.at[i])
                jobs.append((fetch, put))
                at += 16
    for fetch, _ in jobs:
        fetch.start()
    for fetch, put in jobs:
        fetch.wait()
        put.start()
    for _, put in jobs:
        put.wait()


def cut(voltages, plan):
    sizes = [sum(stop - start for (start, stop), _ in pieces) for pieces in plan]
    hbm = pl.BlockSpec(memory_space=pltpu.HBM)
    return pl.pallas_call(
        lambda *refs: cut_kernel(plan, *refs),
        out_shape=[jax.ShapeDtypeStruct((size, NFFT), BF) for size in sizes],
        in_specs=[hbm],
        out_specs=[hbm] * len(plan),
        scratch_shapes=[
            pltpu.VMEM((sum(sizes) // 16, 16, NFFT), BF),
            pltpu.SemaphoreType.DMA((sum(sizes) // 16,)),
            pltpu.SemaphoreType.DMA((sum(sizes) // 16,)),
        ],
        cost_estimate=pl.CostEstimate(flops=10**9, transcendentals=0, bytes_accessed=10**7),
        compiler_params=pltpu.CompilerParams(vmem_limit_bytes=127 * 512 * 1024),
    )(voltages)


def per_device(voltages, pfb_window):
    signals = voltages.shape[0]
    peers = lax.axis_size("ta")
    half = signals // 2
    to_right = [(i, i + 1) for i in range(peers - 1)]
    to_left = [(i, (i - 1) % peers) for i in range(peers)]
    inner = (lax.axis_index("ta") < peers - 1).astype(jnp.int32).reshape(1)
    own = lax.axis_index("aa").astype(jnp.int32).reshape(1)
    to_r, to_l = cut(voltages, ((((0, half), 2),), (((half, signals), 0),)))
    prev_a = lax.ppermute(to_r, "ta", to_right)
    next_b = lax.ppermute(to_l, "ta", to_left)
    top, bottom = (0, half), (half, signals)
    to_r, to_l = cut(voltages, (((top, 1), (bottom, 2)), ((top, 0), (bottom, 1))))
    right = lax.ppermute(to_r, "ta", to_right)
    left = lax.ppermute(to_l, "ta", to_left)
    low = -(half // 16)
    near = ((0, 0), (1, low))
    first = spectra_call(1, first_a, first_b, inner, voltages, (prev_a, next_b), (near,), pfb_window)
    first = lax.all_to_all(first, ("ta", "aa"), split_axis=0, concat_axis=0, tiled=True)
    slots = (near, ((2, 0), (3, 0)), ((3, 0), (2, 0)))
    parts = (prev_a, next_b, left, right)
    second = spectra_call(2, second_a, second_b, inner, voltages, parts, slots, pfb_window)
    second = lax.all_to_all(second, ("ta", "aa"), split_axis=0, concat_axis=0, tiled=True)
    first = spread(first)
    part, send = correlate(own, first, second)
    got = lax.ppermute(send, "aa", [(0, 1), (1, 0)])
    return finish(own, part, got)


def solution(mesh):
    return jax.shard_map(
        per_device,
        mesh=mesh,
        in_specs=(P("aa", "ta"), P()),
        out_specs=P("ta", "aa", None),
        check_vma=False,
    )
```

```python
import math

import jax
import jax.numpy as jnp
import numpy as np
from jax import lax
from jax.experimental import pallas as pl
from jax.experimental.pallas import tpu as pltpu
from jax.sharding import PartitionSpec as P

NFFT = 8192
CH = 2048
TAPS = 4
CH_OFF = 1024
N1 = 64
N2 = 128
NK = 33
NJ = CH // N1
K2 = CH_OFF // N1
HALF = math.sqrt(0.5)
UNROLL = 32
BF = jnp.bfloat16
F32 = jnp.float32


def twiddle_table():
    phase = np.outer(np.arange(NK), np.arange(N2)) * (2.0 * np.pi / NFFT)
    return np.stack([np.cos(phase), np.sin(phase)], axis=1).astype(np.float32)


def bin_table():
    scale = 1.0 / math.sqrt(NFFT)
    bins = np.arange(K2, K2 + NJ)
    rows = []
    for bin_set, sign in ((bins, 1.0), (-(bins + 1), -1.0)):
        phase = np.outer(bin_set, np.arange(N2)) % N2 * (2.0 * np.pi / N2)
        cosine, sine = np.cos(phase) * scale, np.sin(phase) * scale
        rows.append(np.concatenate([cosine, sine], axis=1))
        rows.append(sign * np.concatenate([-sine, cosine], axis=1))
    table = np.concatenate(rows, axis=0)
    high = table.astype(BF)
    low = (table - high.astype(np.float64)).astype(BF)
    return np.concatenate([high, low], axis=0).T


def real_dft8(x):
    s0, d0 = x[0] + x[4], x[0] - x[4]
    s1, d1 = x[1] + x[5], x[1] - x[5]
    s2, d2 = x[2] + x[6], x[2] - x[6]
    s3, d3 = x[3] + x[7], x[3] - x[7]
    e0, e1 = s0 + s2, s1 + s3
    u, v = HALF * (d1 - d3), HALF * (d1 + d3)
    return [(e0 + e1, None), (d0 + u, -(d2 + v)), (s0 - s2, s3 - s1), (d0 - u, d2 - v), (e0 - e1, None)]


def complex_dft8(z, first_half=False):
    sr = [z[j][0] + z[j + 4][0] for j in range(4)]
    si = [z[j][1] + z[j + 4][1] for j in range(4)]
    dr = [z[j][0] - z[j + 4][0] for j in range(4)]
    di = [z[j][1] - z[j + 4][1] for j in range(4)]
    out = [None] * 8
    pr, pi = dr[1], di[1]
    dr[1], di[1] = HALF * (pr + pi), HALF * (pi - pr)
    dr[2], di[2] = di[2], -dr[2]
    pr, pi = dr[3], di[3]
    dr[3], di[3] = HALF * (pi - pr), -HALF * (pr + pi)
    for base, (ar, ai) in ((0, (sr, si)), (1, (dr, di))):
        er, ei = ar[0] + ar[2], ai[0] + ai[2]
        fr, fi = ar[1] + ar[3], ai[1] + ai[3]
        gr, gi = ar[0] - ar[2], ai[0] - ai[2]
        hr, hi = ar[1] - ar[3], ai[1] - ai[3]
        out[base] = (er + fr, ei + fi)
        out[base + 2] = (gr + hi, gi - hr)
        if not first_half:
            out[base + 4] = (er - fr, ei - fi)
            out[base + 6] = (gr - hi, gi + hr)
    return out


def first_half_bins(sections, tw_ref, z_ref, frame, row):
    low_row = row + z_ref.shape[1] // 2

    def keep(k1, re, im, conj):
        c, s = tw_ref[k1, 0:1, :], tw_ref[k1, 1:2, :]
        if im is None:
            zr, zi = re * c, -(re * s)
        elif conj:
            zr, zi = re * c - im * s, -(im * c + re * s)
        else:
            zr, zi = re * c + im * s, im * c - re * s
        for part, z in ((0, zr), (1, zi)):
            high = z.astype(BF)
            low = (z - high.astype(F32)).astype(BF)
            lanes = slice(part * N2, (part + 1) * N2)
            z_ref[k1, pl.ds(pl.multiple_of(row, 16), 16), lanes] = high
            z_ref[k1, pl.ds(pl.multiple_of(low_row, 16), 16), lanes] = low

    spectrum = real_dft8([sections[frame, 0, b] for b in range(8)])
    for r in range(5):
        keep(8 * r, spectrum[r][0], spectrum[r][1], False)
    for q in (1, 2, 3):
        z = []
        for b in range(8):
            re, im = sections[frame, 2 * q - 1, b], sections[frame, 2 * q, b]
            if b:
                c, s = math.cos(2 * math.pi * b * q / N1), math.sin(2 * math.pi * b * q / N1)
                re, im = re * c + im * s, im * c - re * s
            z.append((re, im))
        for r, (re, im) in enumerate(complex_dft8(z)):
            k1 = q + 8 * r
            if k1 <= 32:
                keep(k1, re, im, False)
            else:
                keep(N1 - k1, re, im, True)
    z = []
    for b in range(8):
        x = sections[frame, 7, b]
        c, s = math.cos(2 * math.pi * b * 4 / N1), math.sin(2 * math.pi * b * 4 / N1)
        z.append((x * c, x * -s) if b else (x, jnp.zeros_like(x)))
    out = complex_dft8(z, first_half=True)
    for r in range(4):
        keep(4 + 8 * r, out[r][0], out[r][1], False)


def sections_of(frames_of, n_out, w_ref, sections):
    for b in range(8):
        filtered = [[] for _ in range(n_out)]
        for a in range(8):
            n1 = 8 * a + b
            w = [w_ref[k : k + 1, n1 * N2 : (n1 + 1) * N2] for k in range(TAPS)]
            for f, value in enumerate(frames_of(n1, w)):
                filtered[f].append(value)
        for f in range(n_out):
            spectrum = real_dft8(filtered[f])
            sections[f, 0, b] = spectrum[0][0]
            for q in (1, 2, 3):
                sections[f, 2 * q - 1, b] = spectrum[q][0]
                sections[f, 2 * q, b] = spectrum[q][1]
            sections[f, 7, b] = spectrum[4][0]


def emit_slabs(n_out, table_ref, z_ref, wide_ref, slabs_ref, out_ref, out_sems):
    slab = n_out * 16
    block = 8 * slab
    lap = block + 1
    rows = n_out * N2

    def some(first, count, mirror):
        left = z_ref[pl.ds(first, count)].reshape(count * 2 * rows, 2 * N2)
        product = jnp.dot(left, table_ref[...], preferred_element_type=F32)
        for u in range(count):
            k1 = first + u
            high, low = (product[(2 * u + i) * rows : (2 * u + i + 1) * rows] for i in range(2))
            spectrum = high[:, :N2] + high[:, N2:] + low[:, :N2]
            for f in range(n_out):
                flipped = spectrum[f * N2 : (f + 1) * N2].T
                for side in range(2 if mirror else 1):
                    ch = N1 - k1 if side else k1
                    start = (ch >> 3) * slab + (ch & 7) + f * 16
                    for part in range(2):
                        at = (side * 2 + part) * NJ
                        wide_ref[pl.ds(start + part * 8, NJ, stride=lap), :] = flipped[at : at + NJ]

    some(0, 1, False)
    lax.fori_loop(0, (NK - 1) // UNROLL, lambda i, c: (some(1 + i * UNROLL, UNROLL, True), c)[1], 0)

    def copy_out(j):
        rows = pl.ds(pl.multiple_of(j * block, block), block)
        return pltpu.make_async_copy(slabs_ref.at[rows], out_ref.at[rows], out_sems.at[j])

    def narrow(j, carry):
        slabs_ref[pl.ds(pl.multiple_of(j * block, block), block), :] = wide_ref[pl.ds(j * lap, block), :].astype(BF)
        copy_out(j).start()
        return carry

    lax.fori_loop(0, NJ, narrow, 0, unroll=4)

    def drain(j, carry):
        copy_out(j).wait()
        return carry

    lax.fori_loop(0, NJ, drain, 0)


def fft_kernel(n_out, n_parts, slots, taps_a, taps_b, mask_ref, v_hbm, *refs):
    parts, refs = refs[:n_parts], refs[n_parts:]
    w_ref, tw_ref, table_ref, out_ref, v_buf, hist_buf, sections, z, wide, slabs, sems, out_sems = refs
    keep = mask_ref[0].astype(F32)
    groups = v_buf.shape[0] // 16

    def copies(g, side):
        rows = pl.ds(pl.multiple_of(g * 16, 16), 16)
        jobs = [pltpu.make_async_copy(v_hbm.at[rows], v_buf.at[rows], sems.at[0, g])]
        for k, slot in enumerate(slots):
            part, skip = slot[side]
            source = parts[part].at[pl.ds(pl.multiple_of((g + skip) * 16, 16), 16)]
            jobs.append(pltpu.make_async_copy(source, hist_buf.at[k, rows], sems.at[k + 1, g]))
        return jobs

    for g in range(groups):
        for job in copies(g, g // (groups // 2)):
            job.start()

    def run(taps, side):
        def body(g, carry):
            for job in copies(g, side):
                job.wait()
            rows = pl.ds(pl.multiple_of(g * 16, 16), 16)

            def frames_of(n1, w):
                lanes = slice(n1 * N2, (n1 + 1) * N2)
                v = [v_buf[rows, i * NFFT + n1 * N2 : i * NFFT + (n1 + 1) * N2].astype(F32) for i in range(3)]
                h = [hist_buf[k, rows, lanes].astype(F32) for k in range(len(slots))]
                return taps(keep, w, v, h)

            sections_of(frames_of, n_out, w_ref, sections)
            for f in range(n_out):
                first_half_bins(sections, tw_ref, z, f, f * N2 + g * 16)
            return carry

        return body

    lax.fori_loop(0, groups // 2, run(taps_a, 0), 0)
    lax.fori_loop(groups // 2, groups, run(taps_b, 1), 0)
    emit_slabs(n_out, table_ref, z, wide, slabs, out_ref, out_sems)


def first_a(keep, w, v, h):
    return (w[0] * h[0] + w[1] * v[0] + w[2] * v[1] + w[3] * v[2],)


def first_b(keep, w, v, h):
    return (keep * (w[0] * v[0] + w[1] * v[1] + w[2] * v[2]) + w[3] * h[0],)


def second_a(keep, w, v, h):
    near, one_off, two_off = h
    return (
        keep * (w[0] * v[0] + w[1] * v[1] + w[2] * v[2]) + w[3] * one_off,
        w[0] * two_off + w[1] * near + w[2] * v[0] + w[3] * v[1],
    )


def second_b(keep, w, v, h):
    near, one_off, two_off = h
    return (
        w[0] * one_off + w[1] * v[0] + w[2] * v[1] + w[3] * v[2],
        keep * (w[0] * v[1] + w[1] * v[2]) + w[2] * near + w[3] * two_off,
    )


def spectra_call(n_out, taps_a, taps_b, mask, voltages, parts, slots, window):
    signals = voltages.shape[0]
    n_hist = len(slots)
    rows = CH * 2 * n_out
    vmem = pl.BlockSpec(memory_space=pltpu.VMEM)
    hbm = pl.BlockSpec(memory_space=pltpu.HBM)
    return pl.pallas_call(
        lambda *refs: fft_kernel(n_out, len(parts), slots, taps_a, taps_b, *refs),
        out_shape=jax.ShapeDtypeStruct((rows, N2), BF),
        in_specs=[pl.BlockSpec(memory_space=pltpu.SMEM), hbm] + [hbm] * len(parts) + [vmem] * 3,
        out_specs=hbm,
        scratch_shapes=[
            pltpu.VMEM(voltages.shape, BF),
            pltpu.VMEM((n_hist, signals, NFFT), BF),
            pltpu.VMEM((n_out, 8, 8, 16, N2), F32),
            pltpu.VMEM((NK, 2 * n_out * N2, 2 * N2), BF),
            pltpu.VMEM((rows + NJ, N2), F32),
            pltpu.VMEM((rows, N2), BF),
            pltpu.SemaphoreType.DMA((n_hist + 1, signals // 16)),
            pltpu.SemaphoreType.DMA((NJ,)),
        ],
        cost_estimate=pl.CostEstimate(flops=n_out * 10**10, transcendentals=0, bytes_accessed=n_out * 10**7),
        compiler_params=pltpu.CompilerParams(vmem_limit_bytes=127 * 512 * 1024),
    )(mask, voltages, *parts, window, jnp.asarray(twiddle_table()), jnp.asarray(bin_table()))


LAP = 2 * N2 + 1


def spread_kernel(in_ref, out_ref, wide):
    def body(t, carry):
        for src in range(2):
            tile = in_ref[pl.ds(pl.multiple_of((t * 2 + src) * 16, 16), 16), :].astype(F32)
            for part in range(2):
                wide[src, pl.ds(part * N2 + t, 8, stride=LAP), :] = tile[part * 8 : part * 8 + 8]
        return carry

    lax.fori_loop(0, N2, body, 0, unroll=8)
    for ch in range(8):
        for src in range(2):
            out_ref[ch, :, src * N2 : (src + 1) * N2] = wide[src, ch * LAP : ch * LAP + 2 * N2, :].astype(BF)


def spread(first):
    vmem = pl.BlockSpec(memory_space=pltpu.VMEM)
    return pl.pallas_call(
        spread_kernel,
        out_shape=jax.ShapeDtypeStruct((8, 2 * N2, 2 * N2), BF),
        in_specs=[vmem],
        out_specs=vmem,
        scratch_shapes=[pltpu.VMEM((2, 8 * LAP + 8, N2), F32)],
        cost_estimate=pl.CostEstimate(flops=2 * 10**9, transcendentals=0, bytes_accessed=10**6),
        compiler_params=pltpu.CompilerParams(vmem_limit_bytes=16 * 1024 * 1024),
    )(first)


def correlate_kernel(own_ref, first_ref, second_ref, out_hbm, send_ref, wide, real, imag, rows_buf, sems):
    own = own_ref[0]
    scale = 1.0 / math.sqrt(3 * N2)
    first_lanes = lax.broadcasted_iota(jnp.int32, (16, N2), 1) < N2 // 2

    def body(t, carry):
        for src in range(2):
            for f in range(2):
                row = pl.multiple_of((t * 2 + src) * 32 + f * 16, 16)
                tile = second_ref[pl.ds(row, 16), :].astype(F32)
                if f:
                    row = pl.multiple_of(((t + N2 - 1) % N2 * 2 + src) * 32 + 16, 16)
                    tile = jnp.where(first_lanes, tile, second_ref[pl.ds(row, 16), :].astype(F32))
                for part in range(2):
                    wide[f, src, pl.ds(part * N2 + t, 8, stride=LAP), :] = tile[part * 8 : part * 8 + 8]
        return carry

    lax.fori_loop(0, N2, body, 0, unroll=8)

    first = own == 0
    mine = pl.ds(pl.multiple_of(own * N2, N2), N2)
    theirs = pl.ds(pl.multiple_of((1 - own) * N2, N2), N2)
    upper = lax.broadcasted_iota(jnp.int32, (N2, N2), 0) <= lax.broadcasted_iota(jnp.int32, (N2, N2), 1)
    half_lanes = lax.broadcasted_iota(jnp.int32, (2 * N2, 2 * N2), 1) % N2 < N2 // 2
    dims = (((0,), (0,)), ((), ()))

    def copy_out(ch):
        return pltpu.make_async_copy(rows_buf.at[ch], out_hbm.at[own * 8 + ch], sems.at[ch])

    for ch in range(8):
        rows = slice(ch * LAP, ch * LAP + 2 * N2)
        g1, g2 = (
            jnp.concatenate([wide[f, 0, rows, :].astype(BF), wide[f, 1, rows, :].astype(BF)], axis=1)
            for f in range(2)
        )
        g0 = first_ref[ch]
        x = [jnp.where(half_lanes, g0, g1), jnp.where(half_lanes, g1, g0), g2]
        xr = jnp.concatenate([part[:N2] for part in x], axis=0)
        xi = jnp.concatenate([part[N2:] for part in x], axis=0)
        both = jnp.concatenate([xr, xi], axis=0)
        p = lax.dot_general(xi, xr, dims, preferred_element_type=F32) * scale
        real[...] = lax.dot_general(both, both, dims, preferred_element_type=F32) * scale
        imag[...] = p - p.T
        rows_buf[ch, :, : 2 * N2] = real[mine, :]
        rows_buf[ch, :, 2 * N2 :] = imag[mine, :]
        copy_out(ch).start()
        rows_r, rows_i = real[theirs, :], imag[theirs, :]
        cross_r = jnp.where(first, rows_r[:, :N2], rows_r[:, N2:])
        cross_i = jnp.where(first, rows_i[:, :N2], rows_i[:, N2:])
        diag_r = jnp.where(first, rows_r[:, N2:], rows_r[:, :N2])
        diag_i = jnp.where(first, rows_i[:, N2:], rows_i[:, :N2])
        send_ref[ch, :, :N2] = cross_r.astype(BF)
        send_ref[ch, :, N2 : 2 * N2] = cross_i.astype(BF)
        send_ref[ch, :, 2 * N2 :] = jnp.where(upper, diag_r, diag_i).astype(BF)

    for ch in range(8):
        copy_out(ch).wait()


def correlate(own, first, second):
    vmem = pl.BlockSpec(memory_space=pltpu.VMEM)
    return pl.pallas_call(
        correlate_kernel,
        out_shape=[
            jax.ShapeDtypeStruct((16, N2, 4 * N2), F32),
            jax.ShapeDtypeStruct((8, N2, 3 * N2), BF),
        ],
        in_specs=[pl.BlockSpec(memory_space=pltpu.SMEM), vmem, vmem],
        out_specs=[pl.BlockSpec(memory_space=pltpu.HBM), vmem],
        scratch_shapes=[
            pltpu.VMEM((2, 2, 8 * LAP + 8, N2), F32),
            pltpu.VMEM((2 * N2, 2 * N2), F32),
            pltpu.VMEM((2 * N2, 2 * N2), F32),
            pltpu.VMEM((8, N2, 4 * N2), F32),
            pltpu.SemaphoreType.DMA((8,)),
        ],
        cost_estimate=pl.CostEstimate(flops=5 * 10**9, transcendentals=0, bytes_accessed=10**7),
        compiler_params=pltpu.CompilerParams(vmem_limit_bytes=40 * 1024 * 1024),
    )(own, first, second)


def finish_kernel(own_ref, part_ref, got_ref, out_hbm, rows_buf, sems):
    own = own_ref[0]
    first = own == 0
    row = lax.broadcasted_iota(jnp.int32, (N2, N2), 0)
    col = lax.broadcasted_iota(jnp.int32, (N2, N2), 1)

    def copy_out(ch):
        return pltpu.make_async_copy(rows_buf.at[ch], out_hbm.at[(1 - own) * 8 + ch], sems.at[ch])

    for ch in range(8):
        cross_r = got_ref[ch, :, :N2].astype(F32)
        cross_i = got_ref[ch, :, N2 : 2 * N2].astype(F32)
        packed = got_ref[ch, :, 2 * N2 :].astype(F32)
        flipped = packed.T
        diag_r = jnp.where(row <= col, packed, flipped)
        diag_i = jnp.where(row > col, packed, jnp.where(row < col, -flipped, 0.0))
        rows_buf[ch, :, :N2] = jnp.where(first, diag_r, cross_r)
        rows_buf[ch, :, N2 : 2 * N2] = jnp.where(first, cross_r, diag_r)
        rows_buf[ch, :, 2 * N2 : 3 * N2] = jnp.where(first, diag_i, cross_i)
        rows_buf[ch, :, 3 * N2 :] = jnp.where(first, cross_i, diag_i)
        copy_out(ch).start()
    for ch in range(8):
        copy_out(ch).wait()


def finish(own, part, got):
    return pl.pallas_call(
        finish_kernel,
        out_shape=jax.ShapeDtypeStruct(part.shape, F32),
        in_specs=[
            pl.BlockSpec(memory_space=pltpu.SMEM),
            pl.BlockSpec(memory_space=pltpu.HBM),
            pl.BlockSpec(memory_space=pltpu.VMEM),
        ],
        out_specs=pl.BlockSpec(memory_space=pltpu.HBM),
        scratch_shapes=[pltpu.VMEM((8, N2, 4 * N2), F32), pltpu.SemaphoreType.DMA((8,))],
        input_output_aliases={1: 0},
        compiler_params=pltpu.CompilerParams(vmem_limit_bytes=8 * 1024 * 1024),
    )(own, part, got)


def cut_kernel(plan, v_hbm, *refs):
    outs, (buf, in_sems, out_sems) = refs[: len(plan)], refs[len(plan) :]
    jobs = []
    for out, pieces in zip(outs, plan):
        at = 0
        for (start, stop), frame in pieces:
            for row in range(start, stop, 16):
                i = len(jobs)
                source = v_hbm.at[pl.ds(row, 16), pl.ds(frame * NFFT, NFFT)]
                fetch = pltpu.make_async_copy(source, buf.at[i], in_sems.at[i])
                put = pltpu.make_async_copy(buf.at[i], out.at[pl.ds(at, 16)], out_sems.at[i])
                jobs.append((fetch, put))
                at += 16
    for fetch, _ in jobs:
        fetch.start()
    for fetch, put in jobs:
        fetch.wait()
        put.start()
    for _, put in jobs:
        put.wait()


def cut(voltages, plan):
    sizes = [sum(stop - start for (start, stop), _ in pieces) for pieces in plan]
    hbm = pl.BlockSpec(memory_space=pltpu.HBM)
    return pl.pallas_call(
        lambda *refs: cut_kernel(plan, *refs),
        out_shape=[jax.ShapeDtypeStruct((size, NFFT), BF) for size in sizes],
        in_specs=[hbm],
        out_specs=[hbm] * len(plan),
        scratch_shapes=[
            pltpu.VMEM((sum(sizes) // 16, 16, NFFT), BF),
            pltpu.SemaphoreType.DMA((sum(sizes) // 16,)),
            pltpu.SemaphoreType.DMA((sum(sizes) // 16,)),
        ],
        cost_estimate=pl.CostEstimate(flops=10**9, transcendentals=0, bytes_accessed=10**7),
        compiler_params=pltpu.CompilerParams(vmem_limit_bytes=127 * 512 * 1024),
    )(voltages)


def per_device(voltages, pfb_window):
    signals = voltages.shape[0]
    peers = lax.axis_size("ta")
    half = signals // 2
    to_right = [(i, i + 1) for i in range(peers - 1)]
    to_left = [(i, (i - 1) % peers) for i in range(peers)]
    inner = (lax.axis_index("ta") < peers - 1).astype(jnp.int32).reshape(1)
    own = lax.axis_index("aa").astype(jnp.int32).reshape(1)
    to_r, to_l = cut(voltages, ((((0, half), 2),), (((half, signals), 0),)))
    prev_a = lax.ppermute(to_r, "ta", to_right)
    next_b = lax.ppermute(to_l, "ta", to_left)
    top, bottom = (0, half), (half, signals)
    to_r, to_l = cut(voltages, (((top, 1), (bottom, 2)), ((top, 0), (bottom, 1))))
    right = lax.ppermute(to_r, "ta", to_right)
    left = lax.ppermute(to_l, "ta", to_left)
    low = -(half // 16)
    near = ((0, 0), (1, low))
    first = spectra_call(1, first_a, first_b, inner, voltages, (prev_a, next_b), (near,), pfb_window)
    first = lax.all_to_all(first, ("ta", "aa"), split_axis=0, concat_axis=0, tiled=True)
    slots = (near, ((2, 0), (3, 0)), ((3, 0), (2, 0)))
    parts = (prev_a, next_b, left, right)
    second = spectra_call(2, second_a, second_b, inner, voltages, parts, slots, pfb_window)
    second = lax.all_to_all(second, ("ta", "aa"), split_axis=0, concat_axis=0, tiled=True)
    first = spread(first)
    part, send = correlate(own, first, second)
    got = lax.ppermute(send, "aa", [(0, 1), (1, 0)])
    return finish(own, part, got)


def solution(mesh):
    return jax.shard_map(
        per_device,
        mesh=mesh,
        in_specs=(P("aa", "ta"), P()),
        out_specs=P("ta", "aa", None),
        check_vma=False,
    )
```
